32 devices in a mesh: sp: 16 (over z, x, core), tp: 2 (over y).
Axes of the slice: x: 2, y: 2, z: 4, core: 2. Of those that a mesh axis runs over, the one named last changes fastest.
Arguments:
- activations: bfloat16 [2, 2048, 8192], P(None, 'sp', 'tp'), may hold values from -250 to 250
- norm_gain: bfloat16 [8192], P('tp'), may hold values from 0.5 to 1.5
- keep_bits: int32 [2, 2048, 1024], P(None, 'sp', 'tp'), may hold values from 0 to 255, as said below
- key_value_weight: bfloat16 [1024, 8192], P('sp', 'tp'), may hold values from -0.0625 to 0.0625
- queries: bfloat16 [2, 2048, 4096], P('tp', 'sp'), may hold values from -68 to 68
- segment: int32 [4096], replicated, may hold values from 0 to 15, never falling along the last dimension, each value on 1 to 512 neighbouring positions
- cotangent: bfloat16 [2, 2048, 4096], P('tp', 'sp'), may hold values from -12 to 12
Outputs:
- attended: bfloat16 [2, 2048, 4096], P('tp', 'sp')
- grad_queries: bfloat16 [2, 2048, 4096], P('tp', 'sp')
- grad_activations: bfloat16 [2, 2048, 8192], P(None, 'sp', 'tp')
- grad_weight: float32 [1024, 8192], P('sp', 'tp')
- grad_gain: float32 [8192], P('tp')
The draws below stay inside these ranges and needn't reach their ends.
Inputs may be any that keep to these rules, and one draw needn't show every extreme that they name: Bit j of keep_bits[a, b, w] is the keep flag of feature 8 w + j. segment numbers never fall along the sequence; each document covers 1 to 512 positions, and one covers exactly 512.
All inputs are finite; a program needn't handle non-finite values.
Results may differ from the reference program's by a relative error of at most 0.012.
The reference program's roundings to bfloat16 on the way count: a program that leaves them out, or rounds other values in their place, can miss the bound.
Values may be sent and summed in bfloat16 or wider, within the bound.
A program may use at most 128 MiB of HBM per device.

```python
import math
import jax
import jax.numpy as jnp
import numpy as np
from jax import lax

D = 8192
HQ = 32
KVH = 4
HD = 128
DOC = 512
GROUP = 8
KVC = 1024
BLOCKS = 2
BROWS = 2048
SEQ = 4096


def draw_activations(key, part):
    subkeys = jax.random.split(jax.random.fold_in(key, 11), 3)
    slope_axis = jnp.linspace(0.0, 1.0, D, dtype=jnp.float32)
    values = jnp.clip(jax.random.normal(subkeys[0], (BLOCKS, BROWS, D), jnp.float32), -4.0, 4.0)
    columns = jnp.exp(jnp.log(3.0) * slope_axis + jax.random.uniform(subkeys[1], (D,), jnp.float32, jnp.log(0.5), jnp.log(2.0)))
    row_scale = jnp.exp(jax.random.uniform(subkeys[2], (BLOCKS, BROWS, 1), jnp.float32, 0.0, jnp.log(10.0)))
    return jnp.clip(values * columns * row_scale * 0.5, -250.0, 250.0).astype(jnp.bfloat16)


def draw_keep_bits(key, part):
    packed = jnp.zeros((BLOCKS, BROWS, D // 8), jnp.int32)
    for bit_index in range(8):
        digits = jax.random.randint(jax.random.fold_in(key, 50 + bit_index), (BLOCKS, BROWS, D // 8), 0, 10)
        packed = packed + jnp.left_shift((digits < 9).astype(jnp.int32), bit_index)
    return packed


def draw_queries(key, part):
    subkeys = jax.random.split(jax.random.fold_in(key, 23), 1)
    shape_full = (BLOCKS, BROWS, HQ * HD)
    values = jnp.clip(jax.random.normal(subkeys[0], shape_full, jnp.float32), -4.0, 4.0)
    return values.astype(jnp.bfloat16)


def draw_cotangent(key, part):
    subkeys = jax.random.split(jax.random.fold_in(key, 37), 2)
    shape_full = (BLOCKS, BROWS, HQ * HD)
    position = jnp.linspace(0.0, 1.0, BROWS, dtype=jnp.float32)[None, :, None]
    columns = jnp.exp(jax.random.uniform(subkeys[1], (1, 1, HQ * HD), jnp.float32, jnp.log(0.5), jnp.log(2.0)))
    values = jnp.clip(jax.random.normal(subkeys[0], shape_full, jnp.float32), -4.0, 4.0) * jnp.exp(jnp.log(3.0) * position)
    return jnp.clip(values * columns * 0.5, -12.0, 12.0).astype(jnp.bfloat16)


def block_scale(stream_key, extent, shards, least, high):
    factor_of = 1.0
    for dim, parts in shards:
        steps = jax.random.uniform(jax.random.fold_in(jax.random.fold_in(stream_key, 6), dim), (parts,), jnp.float32, least / len(shards), high / len(shards))
        factor_of = factor_of * jnp.repeat(jnp.exp(steps), extent[dim] // parts).reshape((-1,) + (1,) * (len(extent) - 1 - dim))
    return factor_of


def profile(number_of, total, bound, skew):
    portions = [(1 << 20) // math.isqrt(rank ** skew) + 1 for rank in range(2, number_of + 1)]
    rest, holding = total - bound - (number_of - 1), [1] * (number_of - 1)
    while rest > 0:
        movable = [i for i in range(number_of - 1) if holding[i] < bound]
        pool, left = sum([portions[i] for i in movable]), rest
        for i in movable:
            addition = min(bound - holding[i], max(1, left * portions[i] // pool), rest)
            holding[i] = holding[i] + addition
            rest = rest - addition
    return np.array([bound] + holding)


def ragged_sizes(own_key, number_of, total, bound, lean):
    if number_of == 2:
        one = jax.random.randint(own_key, (), max(1, total - bound), min(bound, total - 1) + 1)
        return jnp.stack([one, total - one])
    lengths = jnp.asarray(profile(number_of, total, bound, lean), jnp.int32)
    twos = (number_of - 1) // 2
    giver, sink = lengths[1:1 + 2 * twos:2], lengths[2:2 + 2 * twos:2]
    slack = jnp.minimum(giver - 1, bound - sink)
    shifted = jax.random.randint(jax.random.fold_in(own_key, 1), (twos,), 0, 1 << 20) % (slack + 1)
    lengths = lengths.at[1:1 + 2 * twos:2].set(giver - shifted).at[2:2 + 2 * twos:2].set(sink + shifted)
    return lengths[jax.random.permutation(jax.random.fold_in(own_key, 2), number_of)]


def bell_draw(own_key, extent, deviation, limit, cuts=(), kind=jnp.bfloat16):
    level = block_scale(own_key, extent, cuts, -0.22, 0.18) if cuts else 1.0
    result = jax.random.normal(own_key, extent, jnp.float32) * deviation * level
    return jnp.minimum(jnp.maximum(result, -limit), limit).astype(kind)


def setup_inputs(seed: int = 0) -> dict:
    streams_of = jax.random.split(jax.random.key(seed), 8)
    return {
        "activations": draw_activations(jax.random.fold_in(streams_of[7], 71), 0),
        "norm_gain": jnp.clip(1.0 + 0.1 * jax.random.normal(streams_of[1], (D,), jnp.float32), 0.5, 1.5).astype(jnp.bfloat16),
        "keep_bits": draw_keep_bits(jax.random.fold_in(streams_of[7], 71), 0),
        "key_value_weight": bell_draw(streams_of[3], (KVC, D), D ** -0.5, 0.0625, ((0, 16), (1, 2))),
        "queries": draw_queries(jax.random.fold_in(streams_of[7], 71), 0),
        "segment": jnp.searchsorted(jnp.cumsum(ragged_sizes(streams_of[5], 2 * SEQ // DOC, SEQ, DOC, 2)), jnp.arange(SEQ), side="right").astype(jnp.int32),
        "cotangent": draw_cotangent(jax.random.fold_in(streams_of[7], 71), 0),
    }


EPS = 1e-05
KEEP_RATE = 0.9
MASKED_SCORE = -1e+30

def unpack_flags(words):
    shifts = jnp.arange(8, dtype=jnp.int32)
    flags = jnp.bitwise_and(jnp.right_shift(words[..., None], shifts), 1)
    return flags.reshape(words.shape[:-1] + (words.shape[-1] * 8,)).astype(jnp.float32)

def group_sum(per_head, group_size):
    row_count, head_count, width = per_head.shape
    summed = lax.optimization_barrier(jnp.sum(per_head.reshape(row_count, head_count // group_size, group_size, width), axis=2))
    return summed.reshape(row_count, head_count // group_size * width).astype(jnp.bfloat16)

def fold_heads(grad_window):
    rounded = lax.optimization_barrier(grad_window.astype(jnp.bfloat16)).astype(jnp.float32)
    return group_sum(rounded, GROUP)

def block_attention(query_block, pair_window, grad_block, allowed):
    score_scale = HD ** (-0.5)
    query_wide = query_block.astype(jnp.float32)
    key_part = pair_window[:, :, :HD].astype(jnp.float32)
    value_part = pair_window[:, :, HD:].astype(jnp.float32)
    grad_wide = grad_block.astype(jnp.float32)
    scores = jnp.einsum('qhd,khd->hqk', query_wide, key_part) * score_scale
    scores = jnp.where(allowed[None], scores, MASKED_SCORE)
    row_max = lax.optimization_barrier(jnp.max(scores, axis=2, keepdims=True))
    weights = jnp.exp(scores - row_max)
    probabilities = weights / lax.optimization_barrier(jnp.sum(weights, axis=2, keepdims=True))
    probs_low = probabilities.astype(jnp.bfloat16)
    probs_back = probs_low.astype(jnp.float32)
    attended = jnp.einsum('hqk,khd->qhd', probs_back, value_part).astype(jnp.bfloat16)
    grad_probs = jnp.einsum('qhd,khd->hqk', grad_wide, value_part)
    row_inner = lax.optimization_barrier(jnp.sum(probabilities * grad_probs, axis=2, keepdims=True))
    grad_scores = (probabilities * (grad_probs - row_inner)).astype(jnp.bfloat16).astype(jnp.float32)
    grad_query = (jnp.einsum('hqk,khd->qhd', grad_scores, key_part) * score_scale).astype(jnp.bfloat16)
    grad_keys = jnp.einsum('hqk,qhd->khd', grad_scores, query_wide) * score_scale
    grad_values = jnp.einsum('hqk,qhd->khd', probs_back, grad_wide)
    return (attended, grad_query, jnp.concatenate([grad_keys, grad_values], axis=2))

def reference(activations, norm_gain, keep_bits, key_value_weight, queries, segment, cotangent):
    gain_wide = norm_gain.astype(jnp.float32)

    def norm_block(inputs):
        row_block, word_block = inputs
        row_wide = row_block.astype(jnp.float32)
        inv_rms = lax.rsqrt(lax.optimization_barrier(jnp.mean(row_wide * row_wide, axis=1, keepdims=True)) + EPS)
        drop_scale = unpack_flags(word_block) / KEEP_RATE
        return ((row_wide * inv_rms * gain_wide * drop_scale).astype(jnp.bfloat16), inv_rms)
    normed, inv_all = lax.map(norm_block, (activations, keep_bits))
    normed_rows = normed.reshape(SEQ, D)
    projected = jnp.dot(normed_rows, key_value_weight.T, preferred_element_type=jnp.float32).astype(jnp.bfloat16)
    pair_heads = jnp.repeat(projected.reshape(SEQ, KVH, 2 * HD), GROUP, axis=1)
    pair_padded = jnp.concatenate([jnp.zeros((DOC, HQ, 2 * HD), jnp.bfloat16), pair_heads], axis=0)
    segment_padded = jnp.concatenate([jnp.full((DOC,), -1, jnp.int32), segment.astype(jnp.int32)])
    query_rows = queries.reshape(SEQ, HQ, HD)
    grad_rows = cotangent.reshape(SEQ, HQ, HD)
    causal = jnp.arange(2 * DOC, dtype=jnp.int32)[None, :] <= jnp.arange(DOC, dtype=jnp.int32)[:, None] + DOC

    def attend_step(pending, block_index):
        offset = (block_index * DOC).astype(jnp.int32)
        query_block = lax.dynamic_slice_in_dim(query_rows, offset, DOC, 0)
        grad_block = lax.dynamic_slice_in_dim(grad_rows, offset, DOC, 0)
        pair_window = lax.dynamic_slice_in_dim(pair_padded, offset, 2 * DOC, 0)
        seg_query = lax.dynamic_slice_in_dim(segment.astype(jnp.int32), offset, DOC, 0)
        seg_keys = lax.dynamic_slice_in_dim(segment_padded, offset, 2 * DOC, 0)
        allowed = causal & (seg_query[:, None] == seg_keys[None, :])
        attended, grad_query, grad_window = block_attention(query_block, pair_window, grad_block, allowed)
        finished = fold_heads(pending + grad_window[:DOC])
        return (grad_window[DOC:], (attended, grad_query, finished))
    final_tail, (outputs, query_grads, finished) = lax.scan(attend_step, jnp.zeros((DOC, HQ, 2 * HD), jnp.float32), jnp.arange(SEQ // DOC, dtype=jnp.int32))
    pair_grads = jnp.concatenate([finished[1:], fold_heads(final_tail)[None]], axis=0).reshape(SEQ, KVC)
    grad_weight = jnp.dot(pair_grads.T, normed_rows, preferred_element_type=jnp.float32) * SEQ ** (-0.5)

    def grad_block_norm(inputs):
        row_block, word_block, inv_rms, grad_pairs = inputs
        row_wide = row_block.astype(jnp.float32)
        drop_scale = unpack_flags(word_block) / KEEP_RATE
        hidden_grad = jnp.dot(grad_pairs, key_value_weight, preferred_element_type=jnp.float32)
        scaled = hidden_grad * drop_scale
        upstream = scaled * gain_wide
        row_dots = lax.optimization_barrier(jnp.sum(upstream * row_wide, axis=1, keepdims=True))
        grad_rows_out = (inv_rms * upstream - row_wide * (inv_rms * inv_rms * inv_rms) * row_dots / D).astype(jnp.bfloat16)
        gain_part = lax.optimization_barrier(jnp.sum(scaled * row_wide * inv_rms, axis=0))
        return (grad_rows_out, gain_part)
    grad_activations, gain_parts = lax.map(grad_block_norm, (activations, keep_bits, inv_all, pair_grads.reshape(BLOCKS, BROWS, KVC)))
    grad_gain = lax.optimization_barrier(jnp.sum(gain_parts, axis=0)) * SEQ ** (-0.5)
    attended = outputs.reshape(BLOCKS, BROWS, HQ * HD)
    grad_queries = query_grads.reshape(BLOCKS, BROWS, HQ * HD)
    return (attended, grad_queries, grad_activations, grad_weight, grad_gain)
```

```python
import functools

import jax
import jax.numpy as jnp
import numpy as np
from jax import lax
from jax.experimental import pallas as pl
from jax.experimental.pallas import tpu as pltpu
from jax.sharding import PartitionSpec as P

D = 8192
HQ = 32
KVH = 4
HD = 128
DOC = 512
GROUP = 8
EPS = 1e-05
KEEP_RATE = 0.9
MASKED_SCORE = -1e30
SCALE = HD ** (-0.5)
DROP = float(np.float32(1.0) / np.float32(KEEP_RATE))
KV = 2 * HD
F32 = jnp.float32
BF16 = jnp.bfloat16
NT = (((1,), (1,)), ((), ()))
TN = (((0,), (0,)), ((), ()))


class Links:
    def __init__(self, send_sems):
        self.send_sems = send_sems
        self.pending = []

    def send(self, cond, src, dst, recv_sem, sp, tp):
        sem = self.send_sems.at[len(self.pending)]

        def make():
            return pltpu.make_async_remote_copy(
                src_ref=src,
                dst_ref=dst,
                send_sem=sem,
                recv_sem=recv_sem,
                device_id={"sp": sp, "tp": tp},
                device_id_type=pl.DeviceIdType.MESH,
            )

        self.pending.append((cond, make))
        when(cond, lambda: make().start())

    def arrive(self, dst, recv_sem, sp, tp):
        pltpu.make_async_remote_copy(
            src_ref=dst,
            dst_ref=dst,
            send_sem=self.send_sems.at[0],
            recv_sem=recv_sem,
            device_id={"sp": sp, "tp": tp},
            device_id_type=pl.DeviceIdType.MESH,
        ).wait_recv()

    def drain(self):
        for cond, make in self.pending:
            when(cond, lambda: make().wait_send())


def when(cond, body):
    if cond is True:
        body()
    else:
        pl.when(cond)(body)


def step_kernel(
    shape, x_ref, gain_ref, bits_ref, w_ref, query_ref, seg_ref, cot_ref,
    att_ref, gq_ref, ga_ref, gw_ref, gg_ref,
    wfull, hall, mask, inv, squares, dots, kvp, kvr, kvh, rim, rimr, own_grad, dkvall, dkt,
    own32, xsend, xr, zs, zru, zrd, ups, gains, probs, grads,
    send_sems, w_sem, w_recv, h_recv, sq_recv, dot_recv, kv_recv, halo_recv, rim_recv, dkv_recv, dkc_recv,
    x_recv, up_recv, down_recv, gain_recv,
):
    S, T, X, Z, rows, F, WR, halo = shape
    R = T * rows
    places = S * T
    sp, tp = lax.axis_index("sp"), lax.axis_index("tp")
    c = sp % 2
    x = sp // 2 % X
    z = sp // (2 * X)
    place = tp * S + sp
    at = lambda zz, xx, cc: (zz * X + xx) * 2 + cc
    mate = at(z, x, 1 - c)
    links = Links(send_sems)

    fetch = pltpu.make_async_copy(w_ref, wfull.at[sp], w_sem)
    fetch.start()
    fetch.wait()

    def spread(cond, zz):
        for k in range(1, X):
            links.send(cond, wfull.at[at(zz, x, c)], wfull.at[at(zz, x, c)], w_recv.at[at(zz, x, c)], at(z, (x + k) % X, c), tp)
        links.send(cond, wfull.at[at(zz, x, c)], wfull.at[at(zz, x, c)], w_recv.at[at(zz, x, c)], mate, tp)

    def pass_on(cond, zz, step):
        block = at(zz, x, c)
        links.send(cond, wfull.at[block], wfull.at[block], w_recv.at[block], at(z + step, x, c), tp)

    pass_on(z < Z - 1, z, 1)
    pass_on(z > 0, z, -1)
    spread(True, z)

    strip = 16
    lanes = F // 128

    def square_rows(i, _):
        r = pl.ds(pl.multiple_of(i * strip, strip), strip)
        wide = x_ref[r, :].astype(F32)
        wide = wide * wide
        total = wide[:, :128]
        for k in range(1, lanes):
            total = total + wide[:, k * 128 : (k + 1) * 128]
        squares[tp, r, :] = total
        return 0

    lax.fori_loop(0, R // strip, square_rows, 0)
    for k in range(1, T):
        links.send(True, squares.at[tp], squares.at[tp], sq_recv.at[tp], sp, (tp + k) % T)

    words = min(128, F // 8)
    lane = lax.broadcasted_iota(jnp.int32, (words, words * 8), 1)
    expand = (lane // 8 == lax.broadcasted_iota(jnp.int32, (words, words * 8), 0)).astype(F32).astype(BF16)
    shifts = lax.broadcasted_iota(jnp.int32, (rows, words * 8), 1) % 8
    for w in range(F // 8 // words):
        def unpack(i, _):
            r = pl.ds(pl.multiple_of(i * rows, rows), rows)
            word = bits_ref[r, w * words : (w + 1) * words].astype(F32).astype(BF16)
            wide = jnp.dot(word, expand, preferred_element_type=F32).astype(jnp.int32)
            flag = jnp.bitwise_and(jnp.right_shift(wide, shifts), 1)
            mask[r, w * words * 8 : (w + 1) * words * 8] = flag.astype(F32).astype(BF16)
            return 0
        lax.fori_loop(0, T, unpack, 0)

    for k in range(1, T):
        links.arrive(squares.at[(tp + k) % T], sq_recv.at[(tp + k) % T], sp, (tp + k) % T)

    def norm_rows(i, _):
        r = pl.ds(pl.multiple_of(i * strip, strip), strip)
        total = squares[0, r, :]
        for t in range(1, T):
            total = total + squares[t, r, :]
        inv_rms = lax.rsqrt(jnp.sum(total, axis=1, keepdims=True) / D + EPS)
        inv[r, :] = jnp.broadcast_to(inv_rms, (strip, 128))
        wide = x_ref[r, :].astype(F32) * inv_rms * gain_ref[...].astype(F32)
        hall[c, r, :] = (wide * (mask[r, :].astype(F32) * DROP)).astype(BF16)
        return 0

    lax.fori_loop(0, R // strip, norm_rows, 0)
    links.send(True, hall.at[c], hall.at[c], h_recv, mate, tp)

    def project(g):
        weight = wfull[pl.ds(g * 2 * X, 2 * X)].reshape(2 * X * WR, F)
        part = lax.dot_general(hall[c], weight, NT, preferred_element_type=F32)
        for t in range(T):
            kvp[g, t] = part[t * rows : (t + 1) * rows]

    def reached(g):
        for k in range(1, X):
            block = at(g, (x + k) % X, c)
            links.arrive(wfull.at[block], w_recv.at[block], mate, tp)

    def across(cond, g):
        for k in range(1, X):
            block = at(g, (x + k) % X, c)
            links.send(cond, wfull.at[block], wfull.at[block], w_recv.at[block], mate, tp)

    def complete(cond, g):
        def body():
            for k in range(X):
                block = at(g, (x + k) % X, 1 - c)
                links.arrive(wfull.at[block], w_recv.at[block], mate, tp)
            project(g)
        when(cond, body)
        for k in range(1, T):
            to = (tp + k) % T
            links.send(cond, kvp.at[g, to], kvr.at[g, tp], kv_recv.at[g, tp], sp, to)

    steps = [(0, 0)] + [(d, s) for d in range(1, Z) for s in (-1, 1)]

    def group_of(step):
        d, s = step
        g = z + d * s
        return (True if d == 0 else (g >= 0) & (g < Z)), g

    for i in range(1, len(steps) + 2):
        if i < len(steps):
            cond, g = group_of(steps[i])
            s = steps[i][1]
            block = at(g, x, c)
            when(cond, lambda: links.arrive(wfull.at[block], w_recv.at[block], mate, tp))
            pass_on(cond & (z - s >= 0) & (z - s < Z), g, -s)
            spread(cond, g)
        if i >= 2:
            cond, g = group_of(steps[i - 2])
            when(cond, lambda: reached(g))
            across(cond, g)
            complete(cond, g)

    for g in range(KVH):
        total = kvp[g, tp]
        for k in range(1, T):
            other = (tp + k) % T
            links.arrive(kvr.at[g, other], kv_recv.at[g, other], sp, other)
            total = total + kvr[g, other]
        kvh[halo, g] = total.astype(BF16)
    for d in range(1, halo + 1):
        to = place + d
        links.send(to < places, kvh.at[halo], kvh.at[halo - d], halo_recv.at[halo - d], to % S, to // S % T)

    def blank(d):
        kvh[halo - d] = jnp.zeros(kvh.shape[1:], BF16)

    for d in range(1, halo + 1):
        pl.when(place < d)(functools.partial(blank, d))
    seg_rows = []
    for j in range(halo + 1):
        back = place - (halo - j)
        row = seg_ref[pl.ds(jnp.maximum(back, 0), 1), :]
        seg_rows.append(jnp.where(back >= 0, row, -1))
    for d in range(1, halo + 1):
        def got(d=d):
            links.arrive(kvh.at[halo - d], halo_recv.at[halo - d], mate, tp)
        pl.when(place >= d)(got)

    keys = rows * (halo + 1)
    seg_keys = jnp.concatenate(seg_rows, axis=1)
    seg_query = jnp.transpose(jnp.broadcast_to(seg_rows[halo].astype(F32), (rows, rows)))[:, :1]
    position = lax.broadcasted_iota(jnp.int32, (rows, keys), 0) + halo * rows
    other = lax.broadcasted_iota(jnp.int32, (rows, keys), 1)
    bias = jnp.where((other <= position) & (seg_query == seg_keys.astype(F32)), 0.0, MASKED_SCORE)

    def attend(g, _):
        pair = kvh[:, g].reshape(keys, KV)
        key_part, value_part = pair[:, :HD], pair[:, HD:]
        queries, cots = [], []
        for n in range(GROUP):
            columns = pl.ds(pl.multiple_of((g * GROUP + n) * HD, HD), HD)
            query, grad = query_ref[:, columns], cot_ref[:, columns]
            queries.append(query)
            cots.append(grad)
            scores = lax.dot_general(query, key_part, NT, preferred_element_type=F32) * SCALE
            scores = jnp.where(bias == 0.0, scores, MASKED_SCORE)
            weights = jnp.exp(scores - jnp.max(scores, axis=1, keepdims=True))
            prob = weights / jnp.sum(weights, axis=1, keepdims=True)
            low = prob.astype(BF16)
            att_ref[:, columns] = jnp.dot(low, value_part, preferred_element_type=F32).astype(BF16)
            grad_prob = lax.dot_general(grad, value_part, NT, preferred_element_type=F32)
            inner = jnp.sum(prob * grad_prob, axis=1, keepdims=True)
            grad_score = (prob * (grad_prob - inner)).astype(BF16)
            gq_ref[:, columns] = (jnp.dot(grad_score, key_part, preferred_element_type=F32) * SCALE).astype(BF16)
            probs[n * rows : (n + 1) * rows, :] = low
            grads[n * rows : (n + 1) * rows, :] = grad_score
        grad_key = lax.dot_general(grads[...], jnp.concatenate(queries, axis=0), TN, preferred_element_type=F32) * SCALE
        grad_value = lax.dot_general(probs[...], jnp.concatenate(cots, axis=0), TN, preferred_element_type=F32)
        for j in range(halo):
            r = slice(j * rows, (j + 1) * rows)
            rim[j, g, :, :HD] = grad_key[r].astype(BF16)
            rim[j, g, :, HD:] = grad_value[r].astype(BF16)
        own_grad[g, :, :HD] = grad_key[halo * rows :]
        own_grad[g, :, HD:] = grad_value[halo * rows :]
        return 0

    lax.fori_loop(0, KVH, attend, 0)

    for d in range(1, halo + 1):
        to = place - d
        links.send(to >= 0, rim.at[halo - d], rimr.at[d - 1], rim_recv.at[d - 1], (to + places) % S, (to + places) // S % T)
    for d in range(1, halo + 1):
        def add(d=d):
            links.arrive(rimr.at[d - 1], rim_recv.at[d - 1], mate, tp)
            for g in range(KVH):
                own_grad[g] = own_grad[g] + rimr[d - 1, g].astype(F32)
        pl.when(place + d < places)(add)
    for g in range(KVH):
        dkvall[c, tp, g] = own_grad[g].astype(BF16)
    for k in range(1, T):
        links.send(True, dkvall.at[c, tp], dkvall.at[c, tp], dkv_recv.at[tp], sp, (tp + k) % T)
    links.send(True, dkvall.at[c, tp], dkvall.at[c, tp], dkc_recv.at[tp], mate, tp)
    for k in range(1, T):
        other = (tp + k) % T
        links.arrive(dkvall.at[c, other], dkv_recv.at[other], sp, other)
        links.send(True, dkvall.at[c, other], dkvall.at[c, other], dkc_recv.at[other], mate, tp)
    for k in range(T):
        other = (tp + k) % T
        links.arrive(dkvall.at[1 - c, other], dkc_recv.at[other], mate, tp)
    links.arrive(hall.at[1 - c], h_recv, mate, tp)

    order = [g for pair in zip(range(Z // 2), range(Z - 1, Z // 2 - 1, -1)) for g in pair]
    tile = min(512, F)
    for g in order:
        dkt[g] = jnp.transpose(dkvall[:, :, g].reshape(2 * R, KV).astype(F32)).astype(BF16)
        left = jnp.concatenate(
            [dkt[g, pl.ds(pl.multiple_of(((x + k) % X * 2 + c) * WR, WR), WR), :] for k in range(X)], axis=0
        )

        def outer(i, _, g=g, left=left):
            columns = pl.ds(pl.multiple_of(i * tile, tile), tile)
            right = hall[:, :, columns].reshape(2 * R, tile)
            part = jnp.dot(left, right, preferred_element_type=F32)
            own32[g, :, columns] = part[:WR]
            for k in range(1, X):
                xsend[g, k - 1, :, columns] = part[k * WR : (k + 1) * WR].astype(BF16)
            return 0

        lax.fori_loop(0, F // tile, outer, 0)
        for k in range(1, X):
            links.send(True, xsend.at[g, k - 1], xr.at[g, k - 1], x_recv.at[g, k - 1], at(z, (x + k) % X, c), tp)

    dkv_mine = jnp.concatenate([dkvall[c, :, g].reshape(R, KV) for g in range(KVH)], axis=1)
    dots[tp] = jnp.zeros((R, 128), F32)
    inv_column = inv[:, :1]

    def hidden(i, _):
        columns = pl.ds(pl.multiple_of(i * tile, tile), tile)
        weight = wfull[:, :, columns].reshape(S * WR, tile)
        scaled = jnp.dot(dkv_mine, weight, preferred_element_type=F32) * (mask[:, columns].astype(F32) * DROP)
        wide = x_ref[:, columns].astype(F32)
        gains[0, :, columns] = jnp.sum(scaled * wide * inv_column, axis=0, keepdims=True)
        upstream = scaled * gain_ref[:, columns].astype(F32)
        ups[:, columns] = upstream
        upstream = upstream * wide
        total = upstream[:, :128]
        for k in range(1, tile // 128):
            total = total + upstream[:, k * 128 : (k + 1) * 128]
        dots[tp] = dots[tp] + total
        return 0

    lax.fori_loop(0, F // tile, hidden, 0)
    for k in range(1, T):
        links.send(True, dots.at[tp], dots.at[tp], dot_recv.at[tp], sp, (tp + k) % T)
    links.send(True, gains.at[0], gains.at[1], gain_recv.at[1], mate, tp)
    links.arrive(gains.at[1], gain_recv.at[1], mate, tp)
    gains[2] = gains[0] + gains[1]
    for k in range(1, X):
        links.send(True, gains.at[2], gains.at[2 + k], gain_recv.at[2 + k], at(z, (x + k) % X, c), tp)
    total = gains[2]
    for k in range(1, X):
        links.arrive(gains.at[2 + k], gain_recv.at[2 + k], mate, tp)
        total = total + gains[2 + k]
    gains[2 + X] = total
    for k in range(1, Z):
        links.send(True, gains.at[2 + X], gains.at[2 + X + k], gain_recv.at[2 + X + k], at((z + k) % Z, x, c), tp)

    for k in range(1, T):
        links.arrive(dots.at[(tp + k) % T], dot_recv.at[(tp + k) % T], sp, (tp + k) % T)

    def finish_rows(i, _):
        r = pl.ds(pl.multiple_of(i * strip, strip), strip)
        total = dots[0, r, :]
        for t in range(1, T):
            total = total + dots[t, r, :]
        row_dot = jnp.sum(total, axis=1, keepdims=True)
        scale = inv[r, :1]
        ga_ref[r, :] = (
            scale * ups[r, :] - x_ref[r, :].astype(F32) * ((scale * scale * scale) * row_dot / D)
        ).astype(BF16)
        return 0

    lax.fori_loop(0, R // strip, finish_rows, 0)

    norm = (places * rows) ** (-0.5)
    for k in range(1, Z):
        links.arrive(gains.at[2 + X + k], gain_recv.at[2 + X + k], mate, tp)
        total = total + gains[2 + X + k]
    gg_ref[...] = total * norm

    def fold(g, extra, out):
        def body(i, _):
            columns = pl.ds(pl.multiple_of(i * tile, tile), tile)
            value = own32[g, :, columns]
            for ref in extra:
                value = value + ref[:, columns].astype(F32)
            out(columns, value)
            return 0
        lax.fori_loop(0, F // tile, body, 0)

    def keep_low(g, columns, value):
        zs[g, :, columns] = value.astype(BF16)

    def keep(g, columns, value):
        own32[g, :, columns] = value

    for g in order:
        for k in range(1, X):
            links.arrive(xr.at[g, k - 1], x_recv.at[g, k - 1], mate, tp)
        parts = [xr.at[g, k - 1] for k in range(1, X)]

        def incoming(ref, sem, g=g, parts=parts):
            links.arrive(ref.at[g], sem.at[g], mate, tp)
            fold(g, parts + [ref.at[g]], functools.partial(keep_low, g))

        pl.when(((z < g) & (z == 0)) | ((z > g) & (z == Z - 1)))(lambda: fold(g, parts, functools.partial(keep_low, g)))
        pl.when((z < g) & (z > 0))(lambda: incoming(zru, up_recv))
        pl.when((z > g) & (z < Z - 1))(lambda: incoming(zrd, down_recv))
        pl.when(z == g)(lambda: fold(g, parts, functools.partial(keep, g)))
        links.send(z < g, zs.at[g], zru.at[g], up_recv.at[g], at(z + 1, x, c), tp)
        links.send(z > g, zs.at[g], zrd.at[g], down_recv.at[g], at(z - 1, x, c), tp)

    def result(columns, value):
        gw_ref[:, columns] = value * norm

    pl.when(z > 0)(lambda: links.arrive(zru.at[z], up_recv.at[z], mate, tp))
    pl.when(z < Z - 1)(lambda: links.arrive(zrd.at[z], down_recv.at[z], mate, tp))
    pl.when(z == 0)(lambda: fold(z, [zrd.at[z]], result))
    pl.when(z == Z - 1)(lambda: fold(z, [zru.at[z]], result))
    pl.when((z > 0) & (z < Z - 1))(lambda: fold(z, [zru.at[z], zrd.at[z]], result))
    links.drain()


def on_device(activations, norm_gain, keep_bits, key_value_weight, queries, segment, cotangent):
    S, T = lax.axis_size("sp"), lax.axis_size("tp")
    blocks, rows, F = activations.shape
    WR = key_value_weight.shape[0]
    Z = KVH
    X = S // (2 * Z)
    R = blocks * rows
    halo = -(-(DOC - 1) // rows)
    keys = rows * (halo + 1)
    shape = (S, T, X, Z, rows, F, WR, halo)
    vmem = pl.BlockSpec(memory_space=pltpu.VMEM)
    dma = pltpu.SemaphoreType.DMA
    wide = queries.shape[-1]
    out = pl.pallas_call(
        functools.partial(step_kernel, shape),
        in_specs=[vmem, vmem, vmem, pl.BlockSpec(memory_space=pl.ANY), vmem, vmem, vmem],
        out_specs=[vmem] * 5,
        out_shape=[
            jax.ShapeDtypeStruct((rows, wide), BF16),
            jax.ShapeDtypeStruct((rows, wide), BF16),
            jax.ShapeDtypeStruct((R, F), BF16),
            jax.ShapeDtypeStruct((WR, F), F32),
            jax.ShapeDtypeStruct((1, F), F32),
        ],
        scratch_shapes=[
            pltpu.VMEM((S, WR, F), BF16),
            pltpu.VMEM((2, R, F), BF16),
            pltpu.VMEM((R, F), BF16),
            pltpu.VMEM((R, 128), F32),
            pltpu.VMEM((T, R, 128), F32),
            pltpu.VMEM((T, R, 128), F32),
            pltpu.VMEM((KVH, T, rows, KV), F32),
            pltpu.VMEM((KVH, T, rows, KV), F32),
            pltpu.VMEM((halo + 1, KVH, rows, KV), BF16),
            pltpu.VMEM((halo, KVH, rows, KV), BF16),
            pltpu.VMEM((halo, KVH, rows, KV), BF16),
            pltpu.VMEM((KVH, rows, KV), F32),
            pltpu.VMEM((2, T, KVH, rows, KV), BF16),
            pltpu.VMEM((KVH, KV, 2 * R), BF16),
            pltpu.VMEM((Z, WR, F), F32),
            pltpu.VMEM((Z, X - 1, WR, F), BF16),
            pltpu.VMEM((Z, X - 1, WR, F), BF16),
            pltpu.VMEM((Z, WR, F), BF16),
            pltpu.VMEM((Z, WR, F), BF16),
            pltpu.VMEM((Z, WR, F), BF16),
            pltpu.VMEM((R, F), F32),
            pltpu.VMEM((2 + X + Z, 1, F), F32),
            pltpu.VMEM((GROUP * rows, keys), BF16),
            pltpu.VMEM((GROUP * rows, keys), BF16),
            dma((240,)),
            dma,
            dma((S,)),
            dma,
            dma((T,)),
            dma((T,)),
            dma((KVH, T)),
            dma((halo,)),
            dma((halo,)),
            dma((T,)),
            dma((T,)),
            dma((Z, X)),
            dma((Z,)),
            dma((Z,)),
            dma((2 + X + Z,)),
        ],
        compiler_params=pltpu.CompilerParams(has_side_effects=True, vmem_limit_bytes=63 * 2**20),
    )(
        activations.reshape(R, F),
        norm_gain.reshape(1, F),
        keep_bits.reshape(R, F // 8),
        key_value_weight,
        queries[0],
        segment.reshape(S * T, rows),
        cotangent[0],
    )
    attended, grad_queries, grad_activations, grad_weight, grad_gain = out
    return (
        attended[None],
        grad_queries[None],
        grad_activations.reshape(activations.shape),
        grad_weight,
        grad_gain.reshape(F),
    )


def solution(mesh):
    return jax.shard_map(
        on_device,
        mesh=mesh,
        in_specs=(
            P(None, "sp", "tp"),
            P("tp"),
            P(None, "sp", "tp"),
            P("sp", "tp"),
            P("tp", "sp", None),
            P(),
            P("tp", "sp", None),
        ),
        out_specs=(
            P("tp", "sp", None),
            P("tp", "sp", None),
            P(None, "sp", "tp"),
            P("sp", "tp"),
            P("tp"),
        ),
        check_vma=False,
    )
```

```python
import functools

import jax
import jax.numpy as jnp
import numpy as np
from jax import lax
from jax.experimental import pallas as pl
from jax.experimental.pallas import tpu as pltpu
from jax.sharding import PartitionSpec as P

D = 8192
HQ = 32
KVH = 4
HD = 128
DOC = 512
GROUP = 8
EPS = 1e-05
KEEP_RATE = 0.9
MASKED_SCORE = -1e30
SCALE = HD ** (-0.5)
DROP = float(np.float32(1.0) / np.float32(KEEP_RATE))
KV = 2 * HD
F32 = jnp.float32
BF16 = jnp.bfloat16
NT = (((1,), (1,)), ((), ()))
UNROLL = 2
TN = (((0,), (0,)), ((), ()))


class Links:
    def __init__(self, send_sems):
        self.send_sems = send_sems
        self.pending = []

    def send(self, cond, src, dst, recv_sem, sp, tp):
        sem = self.send_sems.at[len(self.pending)]

        def make():
            return pltpu.make_async_remote_copy(
                src_ref=src,
                dst_ref=dst,
                send_sem=sem,
                recv_sem=recv_sem,
                device_id={"sp": sp, "tp": tp},
                device_id_type=pl.DeviceIdType.MESH,
            )

        self.pending.append((cond, make))
        when(cond, lambda: make().start())

    def arrive(self, dst, recv_sem, sp, tp):
        pltpu.make_async_remote_copy(
            src_ref=dst,
            dst_ref=dst,
            send_sem=self.send_sems.at[0],
            recv_sem=recv_sem,
            device_id={"sp": sp, "tp": tp},
            device_id_type=pl.DeviceIdType.MESH,
        ).wait_recv()

    def drain(self):
        for cond, make in self.pending:
            when(cond, lambda: make().wait_send())


def when(cond, body):
    if cond is True:
        body()
    else:
        pl.when(cond)(body)


def step_kernel(
    shape, x_ref, gain_ref, bits_ref, w_ref, query_ref, seg_ref, cot_ref,
    att_ref, gq_ref, ga_ref, gw_ref, gg_ref,
    wfull, hall, mask, inv, squares, dots, kvp, kvr, kvh, rim, rimx, rimo, rimr, own_grad, dkvall,
    own32, xsend, xr, zs, zru, zrd, ups, gains, probs, grads,
    send_sems, w_sem, w_recv, h_recv, sq_recv, dot_recv, kv_recv, halo_recv, rimx_recv, rim_recv, dkv_recv, dkc_recv,
    x_recv, up_recv, down_recv, gain_recv,
):
    S, T, X, Z, rows, F, WR, halo = shape
    R = T * rows
    places = S * T
    sp, tp = lax.axis_index("sp"), lax.axis_index("tp")
    c = sp % 2
    x = sp // 2 % X
    z = sp // (2 * X)
    place = tp * S + sp
    at = lambda zz, xx, cc: (zz * X + xx) * 2 + cc
    mate = at(z, x, 1 - c)
    links = Links(send_sems)
    order = [g for pair in zip(range(Z // 2), range(Z - 1, Z // 2 - 1, -1)) for g in pair]
    chunks = WR // 16
    cut = lambda k: pl.ds(k * 16, 16)
    tile = min(512, F)
    strip = 16
    lanes = F // 128

    fetch = pltpu.make_async_copy(w_ref, wfull.at[sp], w_sem)
    fetch.start()
    fetch.wait()

    def move_weight(cond, block, k, to):
        part = wfull.at[block, cut(k)]
        links.send(cond, part, part, w_recv.at[block, k], to, tp)

    def await_weight(cond, block, k):
        when(cond, lambda: links.arrive(wfull.at[block, cut(k)], w_recv.at[block, k], mate, tp))

    def own_up(cond):
        for k in range(chunks):
            move_weight(cond & (z < Z - 1), sp, k, at(z + 1, x, c))

    def own_down(cond):
        for k in range(chunks):
            move_weight(cond & (z > 0), sp, k, at(z - 1, x, c))

    def last_before(g, side):
        ahead = [b for b in order[: order.index(g)] if side(b, g)]
        return ahead[-1] if ahead else None

    up_after = {g: last_before(g, lambda b, a: b < a) for g in range(Z)}
    down_after = {g: last_before(g, lambda b, a: b > a) for g in range(Z)}
    for g in range(Z):
        if up_after[g] is None:
            own_up(z == g)
        if down_after[g] is None:
            own_down(z == g)
    for k in range(chunks):
        for j in range(1, X):
            move_weight(True, sp, k, at(z, (x + j) % X, c))
        move_weight(True, sp, k, mate)

    def weight_in(g, k):
        block = at(g, x, c)
        away = z != g
        await_weight(away, block, k)
        move_weight((z > g) & (z < Z - 1), block, k, at(z + 1, x, c))
        move_weight((z < g) & (z > 0), block, k, at(z - 1, x, c))
        for j in range(1, X):
            move_weight(away, block, k, at(z, (x + j) % X, c))
        move_weight(away, block, k, mate)
        if k == chunks - 1:
            for own in range(Z):
                if up_after[own] == g:
                    own_up(z == own)
                if down_after[own] == g:
                    own_down(z == own)

    def weight_x(g, k):
        for j in range(1, X):
            block = at(g, (x + j) % X, c)
            await_weight(True, block, k)
            move_weight(True, block, k, mate)

    def project(g):
        for k in range(chunks):
            for j in range(X):
                await_weight(True, at(g, j, 1 - c), k)
        weight = wfull[g * 2 * X : (g + 1) * 2 * X].reshape(2 * X * WR, F)
        part = lax.dot_general(hall[c], weight, NT, preferred_element_type=F32)
        for t in range(T):
            kvp[g, t] = part[t * rows : (t + 1) * rows]
        for k in range(1, T):
            to = (tp + k) % T
            links.send(True, kvp.at[g, to], kvr.at[g, tp], kv_recv.at[g, tp], sp, to)

    def square_rows(i, _):
        r = pl.ds(pl.multiple_of(i * strip, strip), strip)
        wide = x_ref[r, :].astype(F32)
        wide = wide * wide
        total = wide[:, :128]
        for k in range(1, lanes):
            total = total + wide[:, k * 128 : (k + 1) * 128]
        squares[tp, r, :] = total
        return 0

    lax.fori_loop(0, R // strip, square_rows, 0)
    for k in range(1, T):
        links.send(True, squares.at[tp], squares.at[tp], sq_recv.at[tp], sp, (tp + k) % T)
    early = chunks // 2
    for k in range(early):
        weight_in(order[0], k)

    words = min(128, F // 8)
    lane = lax.broadcasted_iota(jnp.int32, (words, words * 8), 1)
    expand = (lane // 8 == lax.broadcasted_iota(jnp.int32, (words, words * 8), 0)).astype(F32).astype(BF16)
    shifts = lax.broadcasted_iota(jnp.int32, (rows, words * 8), 1) % 8
    for w in range(F // 8 // words):
        def unpack(i, _):
            r = pl.ds(pl.multiple_of(i * rows, rows), rows)
            word = bits_ref[r, w * words : (w + 1) * words].astype(F32).astype(BF16)
            wide = jnp.dot(word, expand, preferred_element_type=F32).astype(jnp.int32)
            flag = jnp.bitwise_and(jnp.right_shift(wide, shifts), 1)
            mask[r, w * words * 8 : (w + 1) * words * 8] = flag.astype(F32).astype(BF16)
            return 0
        lax.fori_loop(0, T, unpack, 0)

    for k in range(1, T):
        links.arrive(squares.at[(tp + k) % T], sq_recv.at[(tp + k) % T], sp, (tp + k) % T)

    def norm_rows(i, _):
        r = pl.ds(pl.multiple_of(i * strip, strip), strip)
        total = squares[0, r, :]
        for t in range(1, T):
            total = total + squares[t, r, :]
        inv_rms = lax.rsqrt(jnp.sum(total, axis=1, keepdims=True) / D + EPS)
        inv[r, :] = jnp.broadcast_to(inv_rms, (strip, 128))
        wide = x_ref[r, :].astype(F32) * inv_rms * gain_ref[...].astype(F32)
        hall[c, r, :] = (wide * (mask[r, :].astype(F32) * DROP)).astype(BF16)
        return 0

    lax.fori_loop(0, R // strip, norm_rows, 0)
    for k in range(early, chunks):
        weight_in(order[0], k)
    links.send(True, hall.at[c], hall.at[c], h_recv, mate, tp)

    zero = lambda ref: (lambda: ref.__setitem__(Ellipsis, jnp.zeros(ref.shape, ref.dtype)))
    for slot in range(halo):
        pl.when(place + slot < halo)(zero(kvh.at[slot]))
    half = halo // 2
    for g in range(KVH):
        pl.when(c == 0)(zero(rimx.at[g, 0]))
        pl.when(c == 1)(zero(rimx.at[g, half]))
    keys = rows * (halo + 1)
    seg_rows = []
    for j in range(halo + 1):
        back = place - (halo - j)
        row = seg_ref[pl.ds(jnp.maximum(back, 0), 1), :]
        seg_rows.append(jnp.where(back >= 0, row, -1))
    seg_keys = jnp.concatenate(seg_rows, axis=1)
    seg_query = jnp.transpose(jnp.broadcast_to(seg_rows[halo].astype(F32), (rows, rows)))[:, :1]
    position = lax.broadcasted_iota(jnp.int32, (rows, keys), 0) + halo * rows
    other = lax.broadcasted_iota(jnp.int32, (rows, keys), 1)
    bias = jnp.where((other <= position) & (seg_query == seg_keys.astype(F32)), 0.0, MASKED_SCORE)

    def sum_pairs(g):
        total = kvp[g, tp]
        for k in range(1, T):
            other = (tp + k) % T
            links.arrive(kvr.at[g, other], kv_recv.at[g, other], sp, other)
            total = total + kvr[g, other]
        kvh[halo, g] = total.astype(BF16)
        for d in range(1, half + 1):
            to = place + 2 * d
            links.send(to < places, kvh.at[halo, g], kvh.at[halo - 2 * d, g], halo_recv.at[halo - 2 * d, g], to % S, to // S % T)
        links.send(c == 0, kvh.at[halo, g], kvh.at[halo - 1, g], halo_recv.at[halo - 1, g], mate, tp)

    def share_pairs(g):
        for d in range(1, half + 1):
            slot = halo - 2 * d
            here = place >= 2 * d
            when(here, lambda: links.arrive(kvh.at[slot, g], halo_recv.at[slot, g], mate, tp))
            links.send(here & (c == 1), kvh.at[slot, g], kvh.at[slot + 1, g], halo_recv.at[slot + 1, g], mate, tp)
            if slot > 0:
                links.send(here & (c == 0), kvh.at[slot, g], kvh.at[slot - 1, g], halo_recv.at[slot - 1, g], mate, tp)

    def await_pairs(g):
        for slot in range(1, halo, 2):
            when(place + slot >= halo, lambda: links.arrive(kvh.at[slot, g], halo_recv.at[slot, g], mate, tp))

    def attend(g, part):
        heads = GROUP // 2

        def head(i, _):
            n = part * heads + i
            pair = kvh[:, g].reshape(keys, KV)
            key_part, value_part = pair[:, :HD], pair[:, HD:]
            columns = pl.ds(pl.multiple_of((g * GROUP + n) * HD, HD), HD)
            below = pl.ds(pl.multiple_of(n * rows, rows), rows)
            query, grad = query_ref[:, columns], cot_ref[:, columns]
            scores = lax.dot_general(query, key_part, NT, preferred_element_type=F32) * SCALE
            scores = jnp.where(bias == 0.0, scores, MASKED_SCORE)
            weights = jnp.exp(scores - jnp.max(scores, axis=1, keepdims=True))
            prob = weights / jnp.sum(weights, axis=1, keepdims=True)
            low = prob.astype(BF16)
            att_ref[:, columns] = jnp.dot(low, value_part, preferred_element_type=F32).astype(BF16)
            grad_prob = lax.dot_general(grad, value_part, NT, preferred_element_type=F32)
            inner = jnp.sum(prob * grad_prob, axis=1, keepdims=True)
            grad_score = (prob * (grad_prob - inner)).astype(BF16)
            gq_ref[:, columns] = (jnp.dot(grad_score, key_part, preferred_element_type=F32) * SCALE).astype(BF16)
            probs[below, :] = low
            grads[below, :] = grad_score
            return 0

        lax.fori_loop(0, heads, head, 0, unroll=UNROLL)
        if part == 0:
            return
        column = lambda ref, n: ref[:, (g * GROUP + n) * HD : (g * GROUP + n + 1) * HD]
        queries = jnp.concatenate([column(query_ref, n) for n in range(GROUP)], axis=0)
        cots = jnp.concatenate([column(cot_ref, n) for n in range(GROUP)], axis=0)
        grad_key = lax.dot_general(grads[...], queries, TN, preferred_element_type=F32) * SCALE
        grad_value = lax.dot_general(probs[...], cots, TN, preferred_element_type=F32)
        for j in range(halo):
            r = slice(j * rows, (j + 1) * rows)
            rim[g, j, :, :HD] = grad_key[r]
            rim[g, j, :, HD:] = grad_value[r]
        own_grad[g, :, :HD] = grad_key[halo * rows :]
        own_grad[g, :, HD:] = grad_value[halo * rows :]
        for j in range(1, halo, 2):
            low, high = (j - 1) // 2, (j + 1) // 2
            links.send(c == 0, rim.at[g, j], rimx.at[g, low], rimx_recv.at[g, low], mate, tp)
            links.send(c == 1, rim.at[g, j], rimx.at[g, high], rimx_recv.at[g, high], mate, tp)

    def rim_out(g):
        for i in range(half + 1):
            cond = True if 0 < i < half else ((c == 1) if i == 0 else (c == 0))
            when(cond, lambda: links.arrive(rimx.at[g, i], rimx_recv.at[g, i], mate, tp))
        for d in range(1, half + 1):
            slot = halo - 2 * d
            rimo[g, d - 1] = (rim[g, slot] + rimx[g, slot // 2]).astype(BF16)
            to = place - 2 * d
            links.send(to >= 0, rimo.at[g, d - 1], rimr.at[g, d - 1], rim_recv.at[g, d - 1], (to + places) % S, (to + places) // S % T)
        own_grad[g] = own_grad[g] + rimx[g, half]

    def rim_in(g):
        for d in range(1, half + 1):
            def add():
                links.arrive(rimr.at[g, d - 1], rim_recv.at[g, d - 1], mate, tp)
                own_grad[g] = own_grad[g] + rimr[g, d - 1].astype(F32)
            pl.when(place + 2 * d < places)(add)
        dkvall[g, c, tp] = own_grad[g].astype(BF16)
        mine = dkvall.at[g, c, tp]
        for k in range(1, T):
            links.send(True, mine, mine, dkv_recv.at[g, tp], sp, (tp + k) % T)
        links.send(True, mine, mine, dkc_recv.at[g, tp], mate, tp)

    def pair_grads(g):
        for k in range(1, T):
            other = (tp + k) % T
            part = dkvall.at[g, c, other]
            links.arrive(part, dkv_recv.at[g, other], sp, other)
            links.send(True, part, part, dkc_recv.at[g, other], mate, tp)

    def weight_grad(g):
        for t in range(T):
            links.arrive(dkvall.at[g, 1 - c, t], dkc_recv.at[g, t], mate, tp)
        if g == order[0]:
            links.arrive(hall.at[1 - c], h_recv, mate, tp)
        turned = jnp.transpose(dkvall[g].reshape(2 * R, KV).astype(F32))
        rest = turned.reshape(X, 2, WR, 2 * R)
        rest = jnp.where(c == 0, rest[:, 0], rest[:, 1])
        picked = []
        for k in range(X):
            piece = rest[k]
            for j in range(X):
                piece = jnp.where((x + k) % X == j, rest[j], piece)
            picked.append(piece)
        left = jnp.concatenate(picked, axis=0).astype(BF16)

        def outer(i, _):
            columns = pl.ds(pl.multiple_of(i * tile, tile), tile)
            right = hall[:, :, columns].reshape(2 * R, tile)
            part = jnp.dot(left, right, preferred_element_type=F32)
            own32[g, :, columns] = part[:WR]
            for k in range(1, X):
                xsend[g, k - 1, :, columns] = part[k * WR : (k + 1) * WR].astype(BF16)
            return 0

        lax.fori_loop(0, F // tile, outer, 0)
        for q in range(chunks):
            for k in range(1, X):
                links.send(True, xsend.at[g, k - 1, cut(q)], xr.at[g, k - 1, cut(q)], x_recv.at[g, k - 1, q], at(z, (x + k) % X, c), tp)

    def fold(g, k, extra, out):
        def body(i, _):
            columns = pl.ds(pl.multiple_of(i * tile, tile), tile)
            value = own32[g, cut(k), columns]
            for ref in extra:
                value = value + ref[cut(k), columns].astype(F32)
            out(columns, value)
            return 0
        lax.fori_loop(0, F // tile, body, 0)

    def rows_out(g, k):
        for j in range(1, X):
            links.arrive(xr.at[g, j - 1, cut(k)], x_recv.at[g, j - 1, k], mate, tp)
        parts = [xr.at[g, j - 1] for j in range(1, X)]

        def send_low(columns, value):
            zs[g, cut(k), columns] = value.astype(BF16)

        def keep(columns, value):
            own32[g, cut(k), columns] = value

        def incoming(ref, sem):
            links.arrive(ref.at[g, cut(k)], sem.at[g, k], mate, tp)
            fold(g, k, parts + [ref.at[g]], send_low)

        if g > 0:
            pl.when(z == 0)(lambda: fold(g, k, parts, send_low))
            pl.when((z < g) & (z > 0))(lambda: incoming(zru, up_recv))
        if g < Z - 1:
            pl.when(z == Z - 1)(lambda: fold(g, k, parts, send_low))
            pl.when((z > g) & (z < Z - 1))(lambda: incoming(zrd, down_recv))
        pl.when(z == g)(lambda: fold(g, k, parts, keep))
        links.send(z < g, zs.at[g, cut(k)], zru.at[g, cut(k)], up_recv.at[g, k], at(z + 1, x, c), tp)
        links.send(z > g, zs.at[g, cut(k)], zrd.at[g, cut(k)], down_recv.at[g, k], at(z - 1, x, c), tp)

    first, second, third, fourth = order
    for k in range(chunks):
        weight_in(second, k)
        weight_x(first, k)
    project(first)
    for k in range(chunks):
        weight_in(third, k)
        weight_x(second, k)
        if k == 0:
            sum_pairs(first)
        if k == chunks - 1:
            share_pairs(first)
    project(second)
    await_pairs(first)
    attend(first, 0)
    sum_pairs(second)
    for k in range(chunks // 2):
        weight_in(fourth, k)
        weight_x(third, k)
    attend(first, 1)
    share_pairs(second)
    for k in range(chunks // 2, chunks):
        weight_in(fourth, k)
        weight_x(third, k)
    rim_out(first)
    project(third)
    await_pairs(second)
    attend(second, 0)
    sum_pairs(third)
    for k in range(chunks // 2):
        weight_x(fourth, k)
    rim_in(first)
    attend(second, 1)
    share_pairs(third)
    for k in range(chunks // 2, chunks):
        weight_x(fourth, k)
    pair_grads(first)
    rim_out(second)
    project(fourth)
    await_pairs(third)
    attend(third, 0)
    weight_grad(first)
    rim_in(second)
    sum_pairs(fourth)
    attend(third, 1)
    share_pairs(fourth)
    pair_grads(second)
    rim_out(third)
    await_pairs(fourth)
    attend(fourth, 0)
    weight_grad(second)
    rim_in(third)
    attend(fourth, 1)
    pair_grads(third)
    rim_out(fourth)
    for k in range(chunks):
        rows_out(first, k)
    weight_grad(third)
    rim_in(fourth)
    pair_grads(fourth)
    weight_grad(fourth)

    dkv_mine = jnp.concatenate([dkvall[g, c].reshape(R, KV) for g in range(KVH)], axis=1)
    dots[tp] = jnp.zeros((R, 128), F32)
    inv_column = inv[:, :1]

    def hidden(i, _):
        columns = pl.ds(pl.multiple_of(i * tile, tile), tile)
        weight = wfull[:, :, columns].reshape(S * WR, tile)
        scaled = jnp.dot(dkv_mine, weight, preferred_element_type=F32) * (mask[:, columns].astype(F32) * DROP)
        wide = x_ref[:, columns].astype(F32)
        gains[0, :, columns] = jnp.sum(scaled * wide * inv_column, axis=0, keepdims=True)
        upstream = scaled * gain_ref[:, columns].astype(F32)
        ups[:, columns] = upstream
        upstream = upstream * wide
        total = upstream[:, :128]
        for k in range(1, tile // 128):
            total = total + upstream[:, k * 128 : (k + 1) * 128]
        dots[tp] = dots[tp] + total
        return 0

    lax.fori_loop(0, F // tile, hidden, 0)
    for k in range(1, T):
        links.send(True, dots.at[tp], dots.at[tp], dot_recv.at[tp], sp, (tp + k) % T)
    links.send(True, gains.at[0], gains.at[1], gain_recv.at[1], mate, tp)
    for k in range(chunks):
        rows_out(second, k)
    links.arrive(gains.at[1], gain_recv.at[1], mate, tp)
    gains[2] = gains[0] + gains[1]
    for k in range(1, X):
        links.send(True, gains.at[2], gains.at[2 + k], gain_recv.at[2 + k], at(z, (x + k) % X, c), tp)
    for k in range(1, T):
        links.arrive(dots.at[(tp + k) % T], dot_recv.at[(tp + k) % T], sp, (tp + k) % T)

    def finish_rows(i, _):
        r = pl.ds(pl.multiple_of(i * strip, strip), strip)
        total = dots[0, r, :]
        for t in range(1, T):
            total = total + dots[t, r, :]
        row_dot = jnp.sum(total, axis=1, keepdims=True)
        scale = inv[r, :1]
        ga_ref[r, :] = (
            scale * ups[r, :] - x_ref[r, :].astype(F32) * ((scale * scale * scale) * row_dot / D)
        ).astype(BF16)
        return 0

    lax.fori_loop(0, R // strip, finish_rows, 0)
    for k in range(chunks):
        rows_out(third, k)
    for k in range(chunks):
        rows_out(fourth, k)
    total = gains[2]
    for k in range(1, X):
        links.arrive(gains.at[2 + k], gain_recv.at[2 + k], mate, tp)
        total = total + gains[2 + k]
    gains[2 + X] = total
    for k in range(1, Z):
        links.send(True, gains.at[2 + X], gains.at[2 + X + k], gain_recv.at[2 + X + k], at((z + k) % Z, x, c), tp)
    norm = (places * rows) ** (-0.5)

    for k in range(chunks):
        def result(columns, value):
            gw_ref[cut(k), columns] = value * norm

        pl.when(z > 0)(lambda: links.arrive(zru.at[z, cut(k)], up_recv.at[z, k], mate, tp))
        pl.when(z < Z - 1)(lambda: links.arrive(zrd.at[z, cut(k)], down_recv.at[z, k], mate, tp))
        pl.when(z == 0)(lambda: fold(z, k, [zrd.at[z]], result))
        pl.when(z == Z - 1)(lambda: fold(z, k, [zru.at[z]], result))
        pl.when((z > 0) & (z < Z - 1))(lambda: fold(z, k, [zru.at[z], zrd.at[z]], result))
    for k in range(1, Z):
        links.arrive(gains.at[2 + X + k], gain_recv.at[2 + X + k], mate, tp)
        total = total + gains[2 + X + k]
    gg_ref[...] = total * norm
    links.drain()


def on_device(activations, norm_gain, keep_bits, key_value_weight, queries, segment, cotangent):
    S, T = lax.axis_size("sp"), lax.axis_size("tp")
    blocks, rows, F = activations.shape
    WR = key_value_weight.shape[0]
    Z = KVH
    X = S // (2 * Z)
    R = blocks * rows
    halo = 2 * -(-(DOC - 1) // (2 * rows))
    keys = rows * (halo + 1)
    shape = (S, T, X, Z, rows, F, WR, halo)
    vmem = pl.BlockSpec(memory_space=pltpu.VMEM)
    dma = pltpu.SemaphoreType.DMA
    wide = queries.shape[-1]
    out = pl.pallas_call(
        functools.partial(step_kernel, shape),
        in_specs=[vmem, vmem, vmem, pl.BlockSpec(memory_space=pl.ANY), vmem, vmem, vmem],
        out_specs=[vmem] * 5,
        out_shape=[
            jax.ShapeDtypeStruct((rows, wide), BF16),
            jax.ShapeDtypeStruct((rows, wide), BF16),
            jax.ShapeDtypeStruct((R, F), BF16),
            jax.ShapeDtypeStruct((WR, F), F32),
            jax.ShapeDtypeStruct((1, F), F32),
        ],
        scratch_shapes=[
            pltpu.VMEM((S, WR, F), BF16),
            pltpu.VMEM((2, R, F), BF16),
            pltpu.VMEM((R, F), BF16),
            pltpu.VMEM((R, 128), F32),
            pltpu.VMEM((T, R, 128), F32),
            pltpu.VMEM((T, R, 128), F32),
            pltpu.VMEM((KVH, T, rows, KV), F32),
            pltpu.VMEM((KVH, T, rows, KV), F32),
            pltpu.VMEM((halo + 1, KVH, rows, KV), BF16),
            pltpu.VMEM((KVH, halo, rows, KV), F32),
            pltpu.VMEM((KVH, halo // 2 + 1, rows, KV), F32),
            pltpu.VMEM((KVH, halo // 2, rows, KV), BF16),
            pltpu.VMEM((KVH, halo // 2, rows, KV), BF16),
            pltpu.VMEM((KVH, rows, KV), F32),
            pltpu.VMEM((KVH, 2, T, rows, KV), BF16),
            pltpu.VMEM((Z, WR, F), F32),
            pltpu.VMEM((Z, X - 1, WR, F), BF16),
            pltpu.VMEM((Z, X - 1, WR, F), BF16),
            pltpu.VMEM((Z, WR, F), BF16),
            pltpu.VMEM((Z, WR, F), BF16),
            pltpu.VMEM((Z, WR, F), BF16),
            pltpu.VMEM((R, F), F32),
            pltpu.VMEM((2 + X + Z, 1, F), F32),
            pltpu.VMEM((GROUP * rows, keys), BF16),
            pltpu.VMEM((GROUP * rows, keys), BF16),
            dma((500,)),
            dma,
            dma((S, WR // 16)),
            dma,
            dma((T,)),
            dma((T,)),
            dma((KVH, T)),
            dma((halo, KVH)),
            dma((KVH, halo // 2 + 1)),
            dma((KVH, halo // 2)),
            dma((KVH, T)),
            dma((KVH, T)),
            dma((Z, X, WR // 16)),
            dma((Z, WR // 16)),
            dma((Z, WR // 16)),
            dma((2 + X + Z,)),
        ],
        compiler_params=pltpu.CompilerParams(has_side_effects=True, vmem_limit_bytes=63 * 2**20),
    )(
        activations.reshape(R, F),
        norm_gain.reshape(1, F),
        keep_bits.reshape(R, F // 8),
        key_value_weight,
        queries[0],
        segment.reshape(S * T, rows),
        cotangent[0],
    )
    attended, grad_queries, grad_activations, grad_weight, grad_gain = out
    return (
        attended[None],
        grad_queries[None],
        grad_activations.reshape(activations.shape),
        grad_weight,
        grad_gain.reshape(F),
    )


def solution(mesh):
    return jax.shard_map(
        on_device,
        mesh=mesh,
        in_specs=(
            P(None, "sp", "tp"),
            P("tp"),
            P(None, "sp", "tp"),
            P("sp", "tp"),
            P("tp", "sp", None),
            P(),
            P("tp", "sp", None),
        ),
        out_specs=(
            P("tp", "sp", None),
            P("tp", "sp", None),
            P(None, "sp", "tp"),
            P("sp", "tp"),
            P("tp"),
        ),
        check_vma=False,
    )
```

```python
import functools

import jax
import jax.numpy as jnp
import numpy as np
from jax import lax
from jax.experimental import pallas as pl
from jax.experimental.pallas import tpu as pltpu
from jax.sharding import PartitionSpec as P

D = 8192
HQ = 32
KVH = 4
HD = 128
DOC = 512
GROUP = 8
EPS = 1e-05
KEEP_RATE = 0.9
MASKED_SCORE = -1e30
SCALE = HD ** (-0.5)
DROP = float(np.float32(1.0) / np.float32(KEEP_RATE))
KV = 2 * HD
F32 = jnp.float32
BF16 = jnp.bfloat16
NT = (((1,), (1,)), ((), ()))
UNROLL = 2
LOG2E = 1.4426950408889634
TN = (((0,), (0,)), ((), ()))


class Links:
    def __init__(self, send_sems):
        self.send_sems = send_sems
        self.pending = []

    def send(self, cond, src, dst, recv_sem, sp, tp):
        sem = self.send_sems.at[len(self.pending)]

        def make():
            return pltpu.make_async_remote_copy(
                src_ref=src,
                dst_ref=dst,
                send_sem=sem,
                recv_sem=recv_sem,
                device_id={"sp": sp, "tp": tp},
                device_id_type=pl.DeviceIdType.MESH,
            )

        self.pending.append((cond, make))
        when(cond, lambda: make().start())

    def arrive(self, dst, recv_sem, sp, tp):
        pltpu.make_async_remote_copy(
            src_ref=dst,
            dst_ref=dst,
            send_sem=self.send_sems.at[0],
            recv_sem=recv_sem,
            device_id={"sp": sp, "tp": tp},
            device_id_type=pl.DeviceIdType.MESH,
        ).wait_recv()

    def drain(self):
        for cond, make in self.pending:
            when(cond, lambda: make().wait_send())


def when(cond, body):
    if cond is True:
        body()
    else:
        pl.when(cond)(body)


def step_kernel(
    shape, x_hbm, gain_ref, bits_hbm, w_ref, query_hbm, seg_ref, cot_hbm,
    att_hbm, gq_hbm, ga_hbm, gw_hbm, gg_ref,
    x_ref, bits_ref, query_ref, cot_ref, att_ref, gq_ref, ga_ref, gw_ref,
    wfull, hall, mask, inv, squares, dots, kvp, kvr, kvh, rim, rimx, rimo, rimr, own_grad, dkvall,
    own32, xsend, xr, zs, zr, ups, gains, probs, grads, bias,
    send_sems, local_sems, w_recv, h_recv, sq_recv, dot_recv, kv_recv, halo_recv, rimx_recv, rim_recv, dkv_recv, dkc_recv,
    x_recv, z_recv, gain_recv,
):
    S, T, X, Z, rows, F, WR, halo = shape
    R = T * rows
    places = S * T
    sp, tp = lax.axis_index("sp"), lax.axis_index("tp")
    c = sp % 2
    x = sp // 2 % X
    z = sp // (2 * X)
    place = tp * S + sp
    at = lambda zz, xx, cc: (zz * X + xx) * 2 + cc
    mate = at(z, x, 1 - c)
    links = Links(send_sems)
    order = [g for pair in zip(range(Z - 1, Z // 2 - 1, -1), range(Z // 2)) for g in pair]
    chunks = WR // 16
    cut = lambda k: pl.ds(k * 16, 16)
    tile = min(512, F)
    strip = 16
    lanes = F // 128

    inputs = [
        pltpu.make_async_copy(w_ref, wfull.at[sp], local_sems.at[0]),
        pltpu.make_async_copy(x_hbm, x_ref, local_sems.at[1]),
        pltpu.make_async_copy(bits_hbm, bits_ref, local_sems.at[2]),
        pltpu.make_async_copy(query_hbm, query_ref, local_sems.at[3]),
        pltpu.make_async_copy(cot_hbm, cot_ref, local_sems.at[4]),
    ]
    for copy in inputs:
        copy.start()
    results = []

    def put_out(src, dst):
        copy = pltpu.make_async_copy(src, dst, local_sems.at[len(inputs) + len(results)])
        copy.start()
        results.append(copy)

    half = halo // 2
    barrier = pltpu.get_barrier_semaphore()

    def greet(cond, to_sp, to_tp):
        when(cond, lambda: pl.semaphore_signal(
            barrier, inc=1, device_id={"sp": to_sp, "tp": to_tp}, device_id_type=pl.DeviceIdType.MESH
        ))

    for k in range(1, Z):
        greet(True, at((z + k) % Z, x, c), tp)
    for k in range(1, X):
        greet(True, at(z, (x + k) % X, c), tp)
    greet(True, mate, tp)
    for k in range(1, T):
        greet(True, sp, (tp + k) % T)
    greeted = Z - 1 + X - 1 + 1 + T - 1
    for d in range(1, half + 1):
        for to in (place + 2 * d, place - 2 * d):
            inside = (to >= 0) & (to < places)
            greet(inside, (to + places) % S, (to + places) // S % T)
            greeted = greeted + jnp.where(inside, 1, 0)
    pl.semaphore_wait(barrier, greeted)
    inputs[0].wait()

    relayed, direct = order[:2], order[2:]

    def move_weight(cond, block, k, to):
        part = wfull.at[block, cut(k)]
        links.send(cond, part, part, w_recv.at[block, k], to, tp)

    def await_weight(cond, block, k):
        when(cond, lambda: links.arrive(wfull.at[block, cut(k)], w_recv.at[block, k], mate, tp))

    for g in relayed:
        for k in range(chunks):
            if g < Z - 1:
                move_weight(z == g, sp, k, at(z + 1, x, c))
            if g > 0:
                move_weight(z == g, sp, k, at(z - 1, x, c))
            for j in range(1, X):
                move_weight(z == g, sp, k, at(z, (x + j) % X, c))
    for k in range(chunks):
        move_weight(True, sp, k, mate)

    def weight_direct(g, k):
        for d in range(Z - 1, 0, -1):
            for to in (g - d, g + d):
                if 0 <= to < Z:
                    move_weight(z == g, sp, k, at(to, x, c))
        for j in range(1, X):
            move_weight(z == g, sp, k, at(z, (x + j) % X, c))

    def weight_in(g, k, relay=False):
        block = at(g, x, c)
        away = z != g
        await_weight(away, block, k)
        if relay:
            move_weight((z > g) & (z < Z - 1), block, k, at(z + 1, x, c))
            move_weight((z < g) & (z > 0), block, k, at(z - 1, x, c))
        for j in range(1, X):
            move_weight(away, block, k, at(z, (x + j) % X, c))
        move_weight(away, block, k, mate)

    def weight_x(g, k):
        for j in range(1, X):
            block = at(g, (x + j) % X, c)
            await_weight(True, block, k)
            move_weight(True, block, k, mate)

    def project(g):
        for k in range(chunks):
            for j in range(X):
                await_weight(True, at(g, j, 1 - c), k)
        weight = wfull[g * 2 * X : (g + 1) * 2 * X].reshape(2 * X * WR, F)
        part = lax.dot_general(hall[c], weight, NT, preferred_element_type=F32)
        for t in range(T):
            kvp[g, t] = part[t * rows : (t + 1) * rows]
        for k in range(1, T):
            to = (tp + k) % T
            links.send(True, kvp.at[g, to], kvr.at[g, tp], kv_recv.at[g, tp], sp, to)

    def square_rows(i, _):
        r = pl.ds(pl.multiple_of(i * strip, strip), strip)
        wide = x_ref[r, :].astype(F32)
        wide = wide * wide
        total = wide[:, :128]
        for k in range(1, lanes):
            total = total + wide[:, k * 128 : (k + 1) * 128]
        squares[tp, r, :] = total
        return 0

    inputs[1].wait()
    lax.fori_loop(0, R // strip, square_rows, 0)
    for k in range(1, T):
        links.send(True, squares.at[tp], squares.at[tp], sq_recv.at[tp], sp, (tp + k) % T)
    near = jnp.where(z < Z // 2, relayed[1], relayed[0])
    far = jnp.where(z < Z // 2, relayed[0], relayed[1])
    weight_in(near, 0, True)
    inputs[2].wait()
    words = min(128, F // 8)
    lane = lax.broadcasted_iota(jnp.int32, (words, words * 8), 1)
    expand = (lane // 8 == lax.broadcasted_iota(jnp.int32, (words, words * 8), 0)).astype(F32).astype(BF16)
    shifts = lax.broadcasted_iota(jnp.int32, (rows, words * 8), 1) % 8
    for w in range(F // 8 // words):
        def unpack(i, _):
            r = pl.ds(pl.multiple_of(i * rows, rows), rows)
            word = bits_ref[r, w * words : (w + 1) * words].astype(F32).astype(BF16)
            wide = jnp.dot(word, expand, preferred_element_type=F32).astype(jnp.int32)
            flag = jnp.bitwise_and(jnp.right_shift(wide, shifts), 1)
            mask[r, w * words * 8 : (w + 1) * words * 8] = flag.astype(F32).astype(BF16)
            return 0
        lax.fori_loop(0, T, unpack, 0)
    for k in range(1, T):
        links.arrive(squares.at[(tp + k) % T], sq_recv.at[(tp + k) % T], sp, (tp + k) % T)
    weight_in(near, 1, True)
    weight_in(far, 0, True)

    def norm_rows(i, _):
        r = pl.ds(pl.multiple_of(i * strip, strip), strip)
        total = squares[0, r, :]
        for t in range(1, T):
            total = total + squares[t, r, :]
        inv_rms = lax.rsqrt(jnp.sum(total, axis=1, keepdims=True) / D + EPS)
        inv[r, :] = jnp.broadcast_to(inv_rms, (strip, 128))
        wide = x_ref[r, :].astype(F32) * inv_rms * gain_ref[...].astype(F32)
        hall[c, r, :] = (wide * (mask[r, :].astype(F32) * DROP)).astype(BF16)
        return 0

    lax.fori_loop(0, R // strip, norm_rows, 0)
    for k in range(2, chunks):
        weight_in(near, k, True)
        weight_in(far, k - 1, True)
    weight_in(far, chunks - 1, True)
    links.send(True, hall.at[c], hall.at[c], h_recv, mate, tp)

    zero = lambda ref: (lambda: ref.__setitem__(Ellipsis, jnp.zeros(ref.shape, ref.dtype)))
    for slot in range(halo):
        pl.when(place + slot < halo)(zero(kvh.at[slot]))
    for g in range(KVH):
        pl.when(c == 0)(zero(rimx.at[g, 0]))
        pl.when(c == 1)(zero(rimx.at[g, half]))
    keys = rows * (halo + 1)
    seg_rows = []
    for j in range(halo + 1):
        back = place - (halo - j)
        row = seg_ref[pl.ds(jnp.maximum(back, 0), 1), :]
        seg_rows.append(jnp.where(back >= 0, row, -1))
    seg_keys = jnp.concatenate(seg_rows, axis=1)
    seg_query = jnp.transpose(jnp.broadcast_to(seg_rows[halo].astype(F32), (rows, rows)))[:, :1]
    position = lax.broadcasted_iota(jnp.int32, (rows, keys), 0) + halo * rows
    other = lax.broadcasted_iota(jnp.int32, (rows, keys), 1)
    bias[...] = jnp.where((other <= position) & (seg_query == seg_keys.astype(F32)), 0.0, MASKED_SCORE)

    def sum_pairs(g):
        total = kvp[g, tp]
        for k in range(1, T):
            other = (tp + k) % T
            links.arrive(kvr.at[g, other], kv_recv.at[g, other], sp, other)
            total = total + kvr[g, other]
        kvh[halo, g] = total.astype(BF16)
        for d in range(1, half + 1):
            to = place + 2 * d
            links.send(to < places, kvh.at[halo, g], kvh.at[halo - 2 * d, g], halo_recv.at[halo - 2 * d, g], to % S, to // S % T)
        links.send(c == 0, kvh.at[halo, g], kvh.at[halo - 1, g], halo_recv.at[halo - 1, g], mate, tp)

    def share_pairs(g):
        for d in range(1, half + 1):
            slot = halo - 2 * d
            here = place >= 2 * d
            when(here, lambda: links.arrive(kvh.at[slot, g], halo_recv.at[slot, g], mate, tp))
            links.send(here & (c == 1), kvh.at[slot, g], kvh.at[slot + 1, g], halo_recv.at[slot + 1, g], mate, tp)
            if slot > 0:
                links.send(here & (c == 0), kvh.at[slot, g], kvh.at[slot - 1, g], halo_recv.at[slot - 1, g], mate, tp)

    def await_pairs(g):
        for slot in range(1, halo, 2):
            when(place + slot >= halo, lambda: links.arrive(kvh.at[slot, g], halo_recv.at[slot, g], mate, tp))

    def attend(g, part):
        heads = GROUP // 2

        def head(i, _):
            n = part * heads + i
            pair = kvh[:, g].reshape(keys, KV)
            key_part, value_part = pair[:, :HD], pair[:, HD:]
            columns = pl.ds(pl.multiple_of((g * GROUP + n) * HD, HD), HD)
            below = pl.ds(pl.multiple_of(n * rows, rows), rows)
            query, grad = query_ref[:, columns], cot_ref[:, columns]
            scores = lax.dot_general(query, key_part, NT, preferred_element_type=F32) * (SCALE * LOG2E) + bias[...]
            weights = jnp.exp2(scores - jnp.max(scores, axis=1, keepdims=True))
            prob = weights * (1.0 / jnp.sum(weights, axis=1, keepdims=True))
            low = prob.astype(BF16)
            att_ref[:, columns] = jnp.dot(low, value_part, preferred_element_type=F32).astype(BF16)
            grad_prob = lax.dot_general(grad, value_part, NT, preferred_element_type=F32)
            inner = jnp.sum(prob * grad_prob, axis=1, keepdims=True)
            grad_score = (prob * (grad_prob - inner)).astype(BF16)
            gq_ref[:, columns] = (jnp.dot(grad_score, key_part, preferred_element_type=F32) * SCALE).astype(BF16)
            probs[below, :] = low
            grads[below, :] = grad_score
            return 0

        lax.fori_loop(0, heads, head, 0, unroll=UNROLL)
        if part == 0:
            return
        wide = pl.ds(g * GROUP * HD, GROUP * HD)
        put_out(att_ref.at[:, wide], att_hbm.at[:, wide])
        put_out(gq_ref.at[:, wide], gq_hbm.at[:, wide])
        column = lambda ref, n: ref[:, (g * GROUP + n) * HD : (g * GROUP + n + 1) * HD]
        queries = jnp.concatenate([column(query_ref, n) for n in range(GROUP)], axis=0)
        cots = jnp.concatenate([column(cot_ref, n) for n in range(GROUP)], axis=0)
        grad_key = lax.dot_general(grads[...], queries, TN, preferred_element_type=F32) * SCALE
        grad_value = lax.dot_general(probs[...], cots, TN, preferred_element_type=F32)
        for j in range(halo):
            r = slice(j * rows, (j + 1) * rows)
            rim[g, j, :, :HD] = grad_key[r]
            rim[g, j, :, HD:] = grad_value[r]
        own_grad[g, :, :HD] = grad_key[halo * rows :]
        own_grad[g, :, HD:] = grad_value[halo * rows :]
        for j in range(1, halo, 2):
            low, high = (j - 1) // 2, (j + 1) // 2
            links.send(c == 0, rim.at[g, j], rimx.at[g, low], rimx_recv.at[g, low], mate, tp)
            links.send(c == 1, rim.at[g, j], rimx.at[g, high], rimx_recv.at[g, high], mate, tp)

    def rim_out(g):
        for i in range(half + 1):
            cond = True if 0 < i < half else ((c == 1) if i == 0 else (c == 0))
            when(cond, lambda: links.arrive(rimx.at[g, i], rimx_recv.at[g, i], mate, tp))
        for d in range(1, half + 1):
            slot = halo - 2 * d
            rimo[g, d - 1] = (rim[g, slot] + rimx[g, slot // 2]).astype(BF16)
            to = place - 2 * d
            links.send(to >= 0, rimo.at[g, d - 1], rimr.at[g, d - 1], rim_recv.at[g, d - 1], (to + places) % S, (to + places) // S % T)
        own_grad[g] = own_grad[g] + rimx[g, half]

    def rim_in(g):
        for d in range(1, half + 1):
            def add():
                links.arrive(rimr.at[g, d - 1], rim_recv.at[g, d - 1], mate, tp)
                own_grad[g] = own_grad[g] + rimr[g, d - 1].astype(F32)
            pl.when(place + 2 * d < places)(add)
        dkvall[g, c, tp] = own_grad[g].astype(BF16)
        mine = dkvall.at[g, c, tp]
        for k in range(1, T):
            links.send(True, mine, mine, dkv_recv.at[g, tp], sp, (tp + k) % T)
        links.send(True, mine, mine, dkc_recv.at[g, tp], mate, tp)

    def pair_grads(g):
        for k in range(1, T):
            other = (tp + k) % T
            part = dkvall.at[g, c, other]
            links.arrive(part, dkv_recv.at[g, other], sp, other)
            links.send(True, part, part, dkc_recv.at[g, other], mate, tp)

    def weight_grad(g):
        for t in range(T):
            links.arrive(dkvall.at[g, 1 - c, t], dkc_recv.at[g, t], mate, tp)
        if g == order[0]:
            links.arrive(hall.at[1 - c], h_recv, mate, tp)
        turned = jnp.transpose(dkvall[g].reshape(2 * R, KV).astype(F32))
        rest = turned.reshape(X, 2, WR, 2 * R)
        rest = jnp.where(c == 0, rest[:, 0], rest[:, 1])
        picked = []
        for k in range(X):
            piece = rest[k]
            for j in range(X):
                piece = jnp.where((x + k) % X == j, rest[j], piece)
            picked.append(piece)
        left = jnp.concatenate(picked, axis=0).astype(BF16)

        def outer(i, _):
            columns = pl.ds(pl.multiple_of(i * tile, tile), tile)
            right = hall[:, :, columns].reshape(2 * R, tile)
            part = jnp.dot(left, right, preferred_element_type=F32)
            own32[g, :, columns] = part[:WR]
            for k in range(1, X):
                xsend[g, k - 1, :, columns] = part[k * WR : (k + 1) * WR].astype(BF16)
            return 0

        lax.fori_loop(0, F // tile, outer, 0)
        for q in range(chunks):
            for k in range(1, X):
                links.send(True, xsend.at[g, k - 1, cut(q)], xr.at[g, k - 1, cut(q)], x_recv.at[g, k - 1, q], at(z, (x + k) % X, c), tp)

    def fold(g, k, extra, out):
        def body(i, _):
            columns = pl.ds(pl.multiple_of(i * tile, tile), tile)
            value = own32[g, cut(k), columns]
            for ref in extra:
                value = value + ref[cut(k), columns].astype(F32)
            out(columns, value)
            return 0
        lax.fori_loop(0, F // tile, body, 0)

    def rows_out(g, k):
        for j in range(1, X):
            links.arrive(xr.at[g, j - 1, cut(k)], x_recv.at[g, j - 1, k], mate, tp)
        parts = [xr.at[g, j - 1] for j in range(1, X)]

        def send_low(columns, value):
            zs[g, cut(k), columns] = value.astype(BF16)

        def keep(columns, value):
            own32[g, cut(k), columns] = value

        pl.when(z == g)(lambda: fold(g, k, parts, keep))
        pl.when(z != g)(lambda: fold(g, k, parts, send_low))
        links.send(z != g, zs.at[g, cut(k)], zr.at[z, cut(k)], z_recv.at[z, k], at(g, x, c), tp)

    first, second, third, fourth = order
    for k in range(chunks):
        weight_direct(third, k)
        weight_direct(fourth, k)
    inputs[3].wait()
    inputs[4].wait()
    for k in range(chunks):
        weight_x(first, k)
        weight_x(second, k)
    project(first)
    weight_in(third, 0)
    weight_in(third, 1)
    project(second)
    for k in range(2, chunks):
        weight_in(third, k)
        weight_x(third, k - 2)
    weight_in(fourth, 0)
    sum_pairs(first)
    sum_pairs(second)
    for k in range(1, max(chunks - 1, 2)):
        weight_in(fourth, k)
    for k in range(chunks - 2, chunks):
        weight_x(third, k)
    share_pairs(first)
    await_pairs(first)
    attend(first, 0)
    for k in range(max(chunks - 1, 2), chunks):
        weight_in(fourth, k)
    for k in range(chunks - 1):
        weight_x(fourth, k)
    share_pairs(second)
    attend(first, 1)
    weight_x(fourth, chunks - 1)
    await_pairs(second)
    rim_out(first)
    attend(second, 0)
    project(third)
    project(fourth)
    rim_in(first)
    attend(second, 1)
    sum_pairs(third)
    sum_pairs(fourth)
    rim_out(second)
    pair_grads(first)
    weight_grad(first)
    share_pairs(third)
    await_pairs(third)
    attend(third, 0)
    share_pairs(fourth)
    rim_in(second)
    attend(third, 1)
    pair_grads(second)
    weight_grad(second)
    await_pairs(fourth)
    attend(fourth, 0)
    rim_out(third)
    for k in range(chunks):
        rows_out(first, k)
    attend(fourth, 1)
    rim_out(fourth)
    rim_in(third)
    pair_grads(third)
    weight_grad(third)
    for k in range(chunks):
        rows_out(second, k)
    rim_in(fourth)
    pair_grads(fourth)
    weight_grad(fourth)

    dkv_mine = jnp.concatenate([dkvall[g, c].reshape(R, KV) for g in range(KVH)], axis=1)
    dots[tp] = jnp.zeros((R, 128), F32)
    inv_column = inv[:, :1]

    def hidden(i, _):
        columns = pl.ds(pl.multiple_of(i * tile, tile), tile)
        weight = wfull[:, :, columns].reshape(S * WR, tile)
        scaled = jnp.dot(dkv_mine, weight, preferred_element_type=F32) * (mask[:, columns].astype(F32) * DROP)
        wide = x_ref[:, columns].astype(F32)
        gains[0, :, columns] = jnp.sum(scaled * wide * inv_column, axis=0, keepdims=True)
        upstream = scaled * gain_ref[:, columns].astype(F32)
        ups[:, columns] = upstream
        upstream = upstream * wide
        total = upstream[:, :128]
        for k in range(1, tile // 128):
            total = total + upstream[:, k * 128 : (k + 1) * 128]
        dots[tp] = dots[tp] + total
        return 0

    lax.fori_loop(0, F // tile, hidden, 0)
    for k in range(1, T):
        links.send(True, dots.at[tp], dots.at[tp], dot_recv.at[tp], sp, (tp + k) % T)
    links.send(True, gains.at[0], gains.at[1], gain_recv.at[1], mate, tp)
    links.arrive(gains.at[1], gain_recv.at[1], mate, tp)
    gains[2] = gains[0] + gains[1]
    for k in range(1, Z):
        links.send(True, gains.at[2], gains.at[2 + k], gain_recv.at[2 + k], at((z + k) % Z, x, c), tp)
    for k in range(chunks):
        rows_out(third, k)
    total = gains[2]
    for k in range(1, Z):
        links.arrive(gains.at[2 + k], gain_recv.at[2 + k], mate, tp)
        total = total + gains[2 + k]
    gains[2 + Z] = total
    for k in range(1, X):
        links.send(True, gains.at[2 + Z], gains.at[2 + Z + k], gain_recv.at[2 + Z + k], at(z, (x + k) % X, c), tp)
    for k in range(chunks):
        rows_out(fourth, k)
    for k in range(1, T):
        links.arrive(dots.at[(tp + k) % T], dot_recv.at[(tp + k) % T], sp, (tp + k) % T)

    def finish_rows(i, _):
        r = pl.ds(pl.multiple_of(i * strip, strip), strip)
        total = dots[0, r, :]
        for t in range(1, T):
            total = total + dots[t, r, :]
        row_dot = jnp.sum(total, axis=1, keepdims=True)
        scale = inv[r, :1]
        ga_ref[r, :] = (
            scale * ups[r, :] - x_ref[r, :].astype(F32) * ((scale * scale * scale) * row_dot / D)
        ).astype(BF16)
        return 0

    lax.fori_loop(0, R // strip, finish_rows, 0)
    put_out(ga_ref, ga_hbm)
    norm = (places * rows) ** (-0.5)

    for k in range(chunks):
        def result(columns, value):
            gw_ref[cut(k), columns] = value * norm

        sources = [(z + j) % Z for j in range(1, Z)]
        for source in sources:
            links.arrive(zr.at[source, cut(k)], z_recv.at[source, k], mate, tp)
        fold(z, k, [zr.at[source] for source in sources], result)
        put_out(gw_ref.at[cut(k)], gw_hbm.at[cut(k)])
    for k in range(1, X):
        links.arrive(gains.at[2 + Z + k], gain_recv.at[2 + Z + k], mate, tp)
        total = total + gains[2 + Z + k]
    gg_ref[...] = total * norm
    links.drain()
    for copy in results:
        copy.wait()


def on_device(activations, norm_gain, keep_bits, key_value_weight, queries, segment, cotangent):
    S, T = lax.axis_size("sp"), lax.axis_size("tp")
    blocks, rows, F = activations.shape
    WR = key_value_weight.shape[0]
    Z = KVH
    X = S // (2 * Z)
    R = blocks * rows
    halo = 2 * -(-(DOC - 1) // (2 * rows))
    keys = rows * (halo + 1)
    shape = (S, T, X, Z, rows, F, WR, halo)
    vmem = pl.BlockSpec(memory_space=pltpu.VMEM)
    hbm = pl.BlockSpec(memory_space=pl.ANY)
    dma = pltpu.SemaphoreType.DMA
    wide = queries.shape[-1]
    out = pl.pallas_call(
        functools.partial(step_kernel, shape),
        in_specs=[hbm, vmem, hbm, hbm, hbm, vmem, hbm],
        out_specs=[hbm] * 4 + [vmem],
        out_shape=[
            jax.ShapeDtypeStruct((rows, wide), BF16),
            jax.ShapeDtypeStruct((rows, wide), BF16),
            jax.ShapeDtypeStruct((R, F), BF16),
            jax.ShapeDtypeStruct((WR, F), F32),
            jax.ShapeDtypeStruct((1, F), F32),
        ],
        scratch_shapes=[
            pltpu.VMEM((R, F), BF16),
            pltpu.VMEM((R, F // 8), jnp.int32),
            pltpu.VMEM((rows, wide), BF16),
            pltpu.VMEM((rows, wide), BF16),
            pltpu.VMEM((rows, wide), BF16),
            pltpu.VMEM((rows, wide), BF16),
            pltpu.VMEM((R, F), BF16),
            pltpu.VMEM((WR, F), F32),
            pltpu.VMEM((S, WR, F), BF16),
            pltpu.VMEM((2, R, F), BF16),
            pltpu.VMEM((R, F), BF16),
            pltpu.VMEM((R, 128), F32),
            pltpu.VMEM((T, R, 128), F32),
            pltpu.VMEM((T, R, 128), F32),
            pltpu.VMEM((KVH, T, rows, KV), F32),
            pltpu.VMEM((KVH, T, rows, KV), F32),
            pltpu.VMEM((halo + 1, KVH, rows, KV), BF16),
            pltpu.VMEM((KVH, halo, rows, KV), F32),
            pltpu.VMEM((KVH, halo // 2 + 1, rows, KV), F32),
            pltpu.VMEM((KVH, halo // 2, rows, KV), BF16),
            pltpu.VMEM((KVH, halo // 2, rows, KV), BF16),
            pltpu.VMEM((KVH, rows, KV), F32),
            pltpu.VMEM((KVH, 2, T, rows, KV), BF16),
            pltpu.VMEM((Z, WR, F), F32),
            pltpu.VMEM((Z, X - 1, WR, F), BF16),
            pltpu.VMEM((Z, X - 1, WR, F), BF16),
            pltpu.VMEM((Z, WR, F), BF16),
            pltpu.VMEM((Z, WR, F), BF16),
            pltpu.VMEM((R, F), F32),
            pltpu.VMEM((2 + X + Z, 1, F), F32),
            pltpu.VMEM((GROUP * rows, keys), BF16),
            pltpu.VMEM((GROUP * rows, keys), BF16),
            pltpu.VMEM((rows, keys), F32),
            dma((500,)),
            dma((32,)),
            dma((S, WR // 16)),
            dma,
            dma((T,)),
            dma((T,)),
            dma((KVH, T)),
            dma((halo, KVH)),
            dma((KVH, halo // 2 + 1)),
            dma((KVH, halo // 2)),
            dma((KVH, T)),
            dma((KVH, T)),
            dma((Z, X, WR // 16)),
            dma((Z, WR // 16)),
            dma((2 + X + Z,)),
        ],
        compiler_params=pltpu.CompilerParams(collective_id=0, has_side_effects=True, vmem_limit_bytes=63 * 2**20),
    )(
        activations.reshape(R, F),
        norm_gain.reshape(1, F),
        keep_bits.reshape(R, F // 8),
        key_value_weight,
        queries[0],
        segment.reshape(S * T, rows),
        cotangent[0],
    )
    attended, grad_queries, grad_activations, grad_weight, grad_gain = out
    return (
        attended[None],
        grad_queries[None],
        grad_activations.reshape(activations.shape),
        grad_weight,
        grad_gain.reshape(F),
    )


def solution(mesh):
    return jax.shard_map(
        on_device,
        mesh=mesh,
        in_specs=(
            P(None, "sp", "tp"),
            P("tp"),
            P(None, "sp", "tp"),
            P("sp", "tp"),
            P("tp", "sp", None),
            P(),
            P("tp", "sp", None),
        ),
        out_specs=(
            P("tp", "sp", None),
            P("tp", "sp", None),
            P(None, "sp", "tp"),
            P("sp", "tp"),
            P("tp"),
        ),
        check_vma=False,
    )
```

```python
import functools

import jax
import jax.numpy as jnp
import numpy as np
from jax import lax
from jax.experimental import pallas as pl
from jax.experimental.pallas import tpu as pltpu
from jax.sharding import PartitionSpec as P

D = 8192
HQ = 32
KVH = 4
HD = 128
DOC = 512
GROUP = 8
EPS = 1e-05
KEEP_RATE = 0.9
MASKED_SCORE = -1e30
SCALE = HD ** (-0.5)
DROP = float(np.float32(1.0) / np.float32(KEEP_RATE))
KV = 2 * HD
F32 = jnp.float32
BF16 = jnp.bfloat16
NT = (((1,), (1,)), ((), ()))
UNROLL = 1
BATCH = 4
LOG2E = 1.4426950408889634
TN = (((0,), (0,)), ((), ()))


class Links:
    def __init__(self, send_sems):
        self.send_sems = send_sems
        self.pending = []
        self.used = 0

    def send(self, cond, src, dst, recv_sem, sp, tp, again=False):
        self.used += not again
        sem = self.send_sems.at[self.used - 1]

        def make():
            return pltpu.make_async_remote_copy(
                src_ref=src,
                dst_ref=dst,
                send_sem=sem,
                recv_sem=recv_sem,
                device_id={"sp": sp, "tp": tp},
                device_id_type=pl.DeviceIdType.MESH,
            )

        self.pending.append((cond, make))
        when(cond, lambda: make().start())

    def arrive(self, dst, recv_sem, sp, tp):
        pltpu.make_async_remote_copy(
            src_ref=dst,
            dst_ref=dst,
            send_sem=self.send_sems.at[0],
            recv_sem=recv_sem,
            device_id={"sp": sp, "tp": tp},
            device_id_type=pl.DeviceIdType.MESH,
        ).wait_recv()

    def drain(self):
        for cond, make in self.pending:
            when(cond, lambda: make().wait_send())


def when(cond, body):
    if cond is True:
        body()
    else:
        pl.when(cond)(body)


def step_kernel(
    shape, x_hbm, gain_ref, bits_hbm, w_ref, query_hbm, seg_ref, cot_hbm,
    att_hbm, gq_hbm, ga_hbm, gw_hbm, gg_ref,
    x_ref, bits_ref, query_ref, cot_ref, att_ref, gq_ref, ga_ref, gw_ref,
    wfull, hall, mask, inv, squares, dots, kvp, kvr, kvh, rim, rimx, rimo, rimr, own_grad, dkvall,
    own32, xsend, xr, zs, zr, za, ups, gains, probs, grads, bias, gain_row,
    send_sems, local_sems, w_recv, h_recv, sq_recv, dot_recv, kv_recv, halo_recv, rimx_recv, rim_recv, dkv_recv, dkc_recv,
    x_recv, z_recv, a_recv, gain_recv,
):
    S, T, X, Z, rows, F, WR, halo = shape
    R = T * rows
    places = S * T
    sp, tp = lax.axis_index("sp"), lax.axis_index("tp")
    c = sp % 2
    x = sp // 2 % X
    z = sp // (2 * X)
    place = tp * S + sp
    at = lambda zz, xx, cc: (zz * X + xx) * 2 + cc
    mate = at(z, x, 1 - c)
    links = Links(send_sems)
    order = [g for pair in zip(range(Z - 1, Z // 2 - 1, -1), range(Z // 2)) for g in pair]
    chunks = WR // 16
    cut = lambda k: pl.ds(k * 16, 16)
    tile = min(512, F)
    strip = 16
    lanes = F // 128

    inputs = [
        pltpu.make_async_copy(w_ref, wfull.at[sp], local_sems.at[0]),
        pltpu.make_async_copy(x_hbm, x_ref, local_sems.at[1]),
        pltpu.make_async_copy(bits_hbm, bits_ref, local_sems.at[2]),
        pltpu.make_async_copy(query_hbm, query_ref, local_sems.at[3]),
        pltpu.make_async_copy(cot_hbm, cot_ref, local_sems.at[4]),
    ]
    for copy in inputs:
        copy.start()
    results = []

    def put_out(src, dst):
        copy = pltpu.make_async_copy(src, dst, local_sems.at[len(inputs) + len(results)])
        copy.start()
        results.append(copy)

    half = halo // 2
    barrier = pltpu.get_barrier_semaphore()

    def greet(cond, to_sp, to_tp):
        when(cond, lambda: pl.semaphore_signal(
            barrier, inc=1, device_id={"sp": to_sp, "tp": to_tp}, device_id_type=pl.DeviceIdType.MESH
        ))

    for k in range(1, Z):
        greet(True, at((z + k) % Z, x, c), tp)
    for k in range(1, X):
        greet(True, at(z, (x + k) % X, c), tp)
    greet(True, mate, tp)
    for k in range(1, T):
        greet(True, sp, (tp + k) % T)
    greeted = Z - 1 + X - 1 + 1 + T - 1
    for d in range(1, half + 1):
        for to in (place + 2 * d, place - 2 * d):
            inside = (to >= 0) & (to < places)
            greet(inside, (to + places) % S, (to + places) // S % T)
            greeted = greeted + jnp.where(inside, 1, 0)
    pl.semaphore_wait(barrier, greeted)
    inputs[0].wait()

    relayed, direct = order[:2], order[2:]

    def move_weight(cond, block, k, to, again=False):
        part = wfull.at[block, cut(k)]
        links.send(cond, part, part, w_recv.at[block, k], to, tp, again)

    def await_weight(cond, block, k):
        when(cond, lambda: links.arrive(wfull.at[block, cut(k)], w_recv.at[block, k], mate, tp))

    for g in relayed:
        for k in range(chunks):
            if g < Z - 1:
                move_weight(z == g, sp, k, at(z + 1, x, c))
            if g > 0:
                move_weight(z == g, sp, k, at(z - 1, x, c))
            for j in range(1, X):
                move_weight(z == g, sp, k, at(z, (x + j) % X, c))
    for k in range(chunks):
        move_weight(True, sp, k, mate)

    def weight_direct(g, k):
        for d in range(Z - 1, 0, -1):
            for to in (g - d, g + d):
                if 0 <= to < Z:
                    move_weight(z == g, sp, k, at(to, x, c))
        for j in range(1, X):
            move_weight(z == g, sp, k, at(z, (x + j) % X, c))

    def weight_in(g, k, relay=False):
        block = at(g, x, c)
        away = z != g
        await_weight(away, block, k)
        if relay:
            move_weight((z > g) & (z < Z - 1), block, k, at(z + 1, x, c))
            move_weight((z < g) & (z > 0), block, k, at(z - 1, x, c), True)
        for j in range(1, X):
            move_weight(away, block, k, at(z, (x + j) % X, c))
        move_weight(away, block, k, mate)

    def weight_x(g, k):
        for j in range(1, X):
            block = at(g, (x + j) % X, c)
            await_weight(True, block, k)
            move_weight(True, block, k, mate)

    def project(g):
        for k in range(chunks):
            for j in range(X):
                await_weight(True, at(g, j, 1 - c), k)
        weight = wfull[g * 2 * X : (g + 1) * 2 * X].reshape(2 * X * WR, F)
        part = lax.dot_general(hall[c], weight, NT, preferred_element_type=F32)
        for t in range(T):
            kvp[g, t] = part[t * rows : (t + 1) * rows]
        for k in range(1, T):
            to = (tp + k) % T
            links.send(True, kvp.at[g, to], kvr.at[g, tp], kv_recv.at[g, tp], sp, to)

    def square_rows(i, _):
        r = pl.ds(pl.multiple_of(i * strip, strip), strip)
        wide = x_ref[r, :].astype(F32)
        wide = wide * wide
        total = wide[:, :128]
        for k in range(1, lanes):
            total = total + wide[:, k * 128 : (k + 1) * 128]
        squares[tp, r, :] = total
        return 0

    inputs[1].wait()
    gain_row[...] = gain_ref[...].astype(F32).reshape(1, F)
    lax.fori_loop(0, R // strip, square_rows, 0)
    for k in range(1, T):
        links.send(True, squares.at[tp], squares.at[tp], sq_recv.at[tp], sp, (tp + k) % T)
    near = jnp.where(z < Z // 2, relayed[1], relayed[0])
    far = jnp.where(z < Z // 2, relayed[0], relayed[1])
    weight_in(near, 0, True)
    inputs[2].wait()
    words = min(128, F // 8)
    lane = lax.broadcasted_iota(jnp.int32, (words, words * 8), 1)
    expand = (lane // 8 == lax.broadcasted_iota(jnp.int32, (words, words * 8), 0)).astype(F32).astype(BF16)
    shifts = lax.broadcasted_iota(jnp.int32, (rows, words * 8), 1) % 8
    for w in range(F // 8 // words):
        def unpack(i, _):
            r = pl.ds(pl.multiple_of(i * rows, rows), rows)
            word = bits_ref[r, w * words : (w + 1) * words].astype(F32).astype(BF16)
            wide = jnp.dot(word, expand, preferred_element_type=F32).astype(jnp.int32)
            flag = jnp.bitwise_and(jnp.right_shift(wide, shifts), 1)
            mask[r, w * words * 8 : (w + 1) * words * 8] = flag.astype(F32).astype(BF16)
            return 0
        lax.fori_loop(0, T, unpack, 0)
    for k in range(1, T):
        links.arrive(squares.at[(tp + k) % T], sq_recv.at[(tp + k) % T], sp, (tp + k) % T)
    weight_in(near, 1, True)
    weight_in(far, 0, True)

    def norm_rows(i, _):
        r = pl.ds(pl.multiple_of(i * strip, strip), strip)
        total = squares[0, r, :]
        for t in range(1, T):
            total = total + squares[t, r, :]
        inv_rms = lax.rsqrt(jnp.sum(total, axis=1, keepdims=True) / D + EPS)
        inv[r, :] = jnp.broadcast_to(inv_rms, (strip, 128))
        wide = x_ref[r, :].astype(F32) * inv_rms * gain_row[...]
        hall[c, r, :] = (wide * (mask[r, :].astype(F32) * DROP)).astype(BF16)
        return 0

    lax.fori_loop(0, R // strip, norm_rows, 0)
    for k in range(2, chunks):
        weight_in(near, k, True)
        weight_in(far, k - 1, True)
    weight_in(far, chunks - 1, True)
    links.send(True, hall.at[c], hall.at[c], h_recv, mate, tp)

    zero = lambda ref: (lambda: ref.__setitem__(Ellipsis, jnp.zeros(ref.shape, ref.dtype)))
    for slot in range(halo):
        pl.when(place + slot < halo)(zero(kvh.at[slot]))
    for g in range(KVH):
        pl.when(c == 0)(zero(rimx.at[g, 0]))
        pl.when(c == 1)(zero(rimx.at[g, half]))
    keys = rows * (halo + 1)
    seg_rows = []
    for j in range(halo + 1):
        back = place - (halo - j)
        row = seg_ref[pl.ds(jnp.maximum(back, 0), 1), :]
        seg_rows.append(jnp.where(back >= 0, row, -1))
    seg_keys = jnp.concatenate(seg_rows, axis=1)
    seg_query = jnp.transpose(jnp.broadcast_to(seg_rows[halo].astype(F32), (rows, rows)))[:, :1]
    position = lax.broadcasted_iota(jnp.int32, (rows, keys), 0) + halo * rows
    other = lax.broadcasted_iota(jnp.int32, (rows, keys), 1)
    bias[...] = jnp.where((other <= position) & (seg_query == seg_keys.astype(F32)), 0.0, MASKED_SCORE)

    def sum_pairs(g):
        total = kvp[g, tp]
        for k in range(1, T):
            other = (tp + k) % T
            links.arrive(kvr.at[g, other], kv_recv.at[g, other], sp, other)
            total = total + kvr[g, other]
        kvh[halo, g] = total.astype(BF16)
        for d in range(1, half + 1):
            to = place + 2 * d
            links.send(to < places, kvh.at[halo, g], kvh.at[halo - 2 * d, g], halo_recv.at[halo - 2 * d, g], to % S, to // S % T)
        links.send(c == 0, kvh.at[halo, g], kvh.at[halo - 1, g], halo_recv.at[halo - 1, g], mate, tp)

    def share_pairs(g):
        for d in range(1, half + 1):
            slot = halo - 2 * d
            here = place >= 2 * d
            when(here, lambda: links.arrive(kvh.at[slot, g], halo_recv.at[slot, g], mate, tp))
            links.send(here & (c == 1), kvh.at[slot, g], kvh.at[slot + 1, g], halo_recv.at[slot + 1, g], mate, tp)
            if slot > 0:
                links.send(here & (c == 0), kvh.at[slot, g], kvh.at[slot - 1, g], halo_recv.at[slot - 1, g], mate, tp, True)

    def await_pairs(g):
        for slot in range(1, halo, 2):
            when(place + slot >= halo, lambda: links.arrive(kvh.at[slot, g], halo_recv.at[slot, g], mate, tp))

    def attend(g, part):
        heads = GROUP // 2

        pair = kvh[:, g].reshape(keys, KV)
        key_part, value_part = pair[:, :HD], pair[:, HD:]

        def some_heads(i, _):
            each = range(BATCH)
            n = [part * heads + i * BATCH + j for j in each]
            columns = [pl.ds(pl.multiple_of((g * GROUP + n[j]) * HD, HD), HD) for j in each]
            query = jnp.concatenate([query_ref[:, columns[j]] for j in each], axis=0)
            grad = jnp.concatenate([cot_ref[:, columns[j]] for j in each], axis=0)
            below = pl.ds(pl.multiple_of(n[0] * rows, rows), BATCH * rows)
            raw = lax.dot_general(query, key_part, NT, preferred_element_type=F32)
            grad_prob = lax.dot_general(grad, value_part, NT, preferred_element_type=F32)
            bias_all = jnp.concatenate([bias[...]] * BATCH, axis=0)
            scores = raw * (SCALE * LOG2E) + bias_all
            weights = jnp.exp2(scores - jnp.max(scores, axis=1, keepdims=True))
            prob = weights * (1.0 / jnp.sum(weights, axis=1, keepdims=True))
            low = prob.astype(BF16)
            probs[below, :] = low
            inner = jnp.sum(prob * grad_prob, axis=1, keepdims=True)
            grad_score = (prob * (grad_prob - inner)).astype(BF16)
            grads[below, :] = grad_score
            out = jnp.dot(low, value_part, preferred_element_type=F32).astype(BF16)
            grad_out = (jnp.dot(grad_score, key_part, preferred_element_type=F32) * SCALE).astype(BF16)
            for j in each:
                att_ref[:, columns[j]] = out[j * rows : (j + 1) * rows]
                gq_ref[:, columns[j]] = grad_out[j * rows : (j + 1) * rows]
            return 0

        lax.fori_loop(0, heads // BATCH, some_heads, 0, unroll=UNROLL)
        if part == 0:
            return
        wide = pl.ds(g * GROUP * HD, GROUP * HD)
        put_out(att_ref.at[:, wide], att_hbm.at[:, wide])
        put_out(gq_ref.at[:, wide], gq_hbm.at[:, wide])
        column = lambda ref, n: ref[:, (g * GROUP + n) * HD : (g * GROUP + n + 1) * HD]
        queries = jnp.concatenate([column(query_ref, n) for n in range(GROUP)], axis=0)
        cots = jnp.concatenate([column(cot_ref, n) for n in range(GROUP)], axis=0)
        grad_key = lax.dot_general(grads[...], queries, TN, preferred_element_type=F32) * SCALE
        grad_value = lax.dot_general(probs[...], cots, TN, preferred_element_type=F32)
        for j in range(halo):
            r = slice(j * rows, (j + 1) * rows)
            rim[g, j, :, :HD] = grad_key[r]
            rim[g, j, :, HD:] = grad_value[r]
        own_grad[g, :, :HD] = grad_key[halo * rows :]
        own_grad[g, :, HD:] = grad_value[halo * rows :]
        for j in range(1, halo, 2):
            low, high = (j - 1) // 2, (j + 1) // 2
            links.send(c == 0, rim.at[g, j], rimx.at[g, low], rimx_recv.at[g, low], mate, tp)
            links.send(c == 1, rim.at[g, j], rimx.at[g, high], rimx_recv.at[g, high], mate, tp, True)

    def rim_out(g):
        for i in range(half + 1):
            cond = True if 0 < i < half else ((c == 1) if i == 0 else (c == 0))
            when(cond, lambda: links.arrive(rimx.at[g, i], rimx_recv.at[g, i], mate, tp))
        for d in range(1, half + 1):
            slot = halo - 2 * d
            rimo[g, d - 1] = (rim[g, slot] + rimx[g, slot // 2]).astype(BF16)
            to = place - 2 * d
            links.send(to >= 0, rimo.at[g, d - 1], rimr.at[g, d - 1], rim_recv.at[g, d - 1], (to + places) % S, (to + places) // S % T)
        own_grad[g] = own_grad[g] + rimx[g, half]

    def rim_in(g):
        for d in range(1, half + 1):
            def add():
                links.arrive(rimr.at[g, d - 1], rim_recv.at[g, d - 1], mate, tp)
                own_grad[g] = own_grad[g] + rimr[g, d - 1].astype(F32)
            pl.when(place + 2 * d < places)(add)
        dkvall[g, c, tp] = own_grad[g].astype(BF16)
        mine = dkvall.at[g, c, tp]
        for k in range(1, T):
            links.send(True, mine, mine, dkv_recv.at[g, tp], sp, (tp + k) % T)
        links.send(True, mine, mine, dkc_recv.at[g, tp], mate, tp)

    def pair_grads(g):
        for k in range(1, T):
            other = (tp + k) % T
            part = dkvall.at[g, c, other]
            links.arrive(part, dkv_recv.at[g, other], sp, other)
            links.send(True, part, part, dkc_recv.at[g, other], mate, tp)

    def weight_grad(g):
        for t in range(T):
            links.arrive(dkvall.at[g, 1 - c, t], dkc_recv.at[g, t], mate, tp)
        if g == order[0]:
            links.arrive(hall.at[1 - c], h_recv, mate, tp)
        turned = jnp.transpose(dkvall[g].reshape(2 * R, KV).astype(F32))
        rest = turned.reshape(X, 2, WR, 2 * R)
        rest = jnp.where(c == 0, rest[:, 0], rest[:, 1])
        picked = []
        for k in range(X):
            piece = rest[k]
            for j in range(X):
                piece = jnp.where((x + k) % X == j, rest[j], piece)
            picked.append(piece)
        left = jnp.concatenate(picked, axis=0).astype(BF16)

        def outer(i, _):
            columns = pl.ds(pl.multiple_of(i * tile, tile), tile)
            right = hall[:, :, columns].reshape(2 * R, tile)
            part = jnp.dot(left, right, preferred_element_type=F32)
            own32[g, :, columns] = part[:WR]
            for k in range(1, X):
                xsend[g, k - 1, :, columns] = part[k * WR : (k + 1) * WR].astype(BF16)
            return 0

        lax.fori_loop(0, F // tile, outer, 0)

    def grads_x(g, pieces):
        for q in pieces:
            for k in range(1, X):
                links.send(True, xsend.at[g, k - 1, cut(q)], xr.at[g, k - 1, cut(q)], x_recv.at[g, k - 1, q], at(z, (x + k) % X, c), tp)

    def fold(g, k, extra, out):
        def body(i, _):
            columns = pl.ds(pl.multiple_of(i * tile, tile), tile)
            value = own32[g, cut(k), columns]
            for ref in extra:
                value = value + ref[cut(k), columns].astype(F32)
            out(columns, value)
            return 0
        lax.fori_loop(0, F // tile, body, 0)

    def rows_out(g, k):
        for j in range(1, X):
            links.arrive(xr.at[g, j - 1, cut(k)], x_recv.at[g, j - 1, k], mate, tp)
        parts = [xr.at[g, j - 1] for j in range(1, X)]

        def send_low(columns, value):
            zs[g, cut(k), columns] = value.astype(BF16)

        def keep(columns, value):
            own32[g, cut(k), columns] = value

        pl.when(z == g)(lambda: fold(g, k, parts, keep))
        if g in relayed:
            pl.when(z != g)(lambda: fold(g, k, parts, send_low))
            links.send(z != g, zs.at[g, cut(k)], zr.at[z, cut(k)], z_recv.at[z, k], at(g, x, c), tp)
            return
        for step, ends, passes in ((1, z == 0, (z > 0) & (z < g)), (-1, z == Z - 1, (z > g) & (z < Z - 1))):
            def add():
                links.arrive(za.at[g, cut(k)], a_recv.at[g, k], mate, tp)
                fold(g, k, parts + [za.at[g]], send_low)

            if (g if step > 0 else Z - 1 - g) > 0:
                pl.when(ends)(lambda: fold(g, k, parts, send_low))
                pl.when(passes)(add)
                going = (z < g) if step > 0 else (z > g)
                last = z + step == g
                links.send(going & last, zs.at[g, cut(k)], zr.at[z, cut(k)], z_recv.at[z, k], at(z + step, x, c), tp)
                links.send(going & (z + step != g), zs.at[g, cut(k)], za.at[g, cut(k)], a_recv.at[g, k], at(z + step, x, c), tp, True)

    first, second, third, fourth = order
    for k in range(chunks):
        weight_direct(third, k)
        weight_direct(fourth, k)
    inputs[3].wait()
    inputs[4].wait()
    for k in range(chunks):
        weight_x(first, k)
        weight_x(second, k)
    project(first)
    weight_in(third, 0)
    weight_in(third, 1)
    project(second)
    sum_pairs(first)
    for k in range(2, chunks - 1):
        weight_in(third, k)
    weight_x(third, 0)
    sum_pairs(second)
    share_pairs(first)
    for k in range(1, chunks // 2):
        weight_x(third, k)
    await_pairs(first)
    attend(first, 0)
    for k in range(max(chunks - 1, 2), chunks):
        weight_in(third, k)
    for k in range(chunks // 2):
        weight_in(fourth, k)
        weight_x(third, chunks // 2 + k)
    share_pairs(second)
    attend(first, 1)
    for k in range(chunks // 2, chunks):
        weight_in(fourth, k)
        weight_x(fourth, k - chunks // 2)
    await_pairs(second)
    rim_out(first)
    attend(second, 0)
    project(third)
    for k in range(chunks - chunks // 2, chunks):
        weight_x(fourth, k)
    rim_in(first)
    project(fourth)
    attend(second, 1)
    sum_pairs(third)
    sum_pairs(fourth)
    rim_out(second)
    pair_grads(first)
    weight_grad(first)
    share_pairs(third)
    grads_x(first, range(chunks // 2))
    await_pairs(third)
    attend(third, 0)
    share_pairs(fourth)
    grads_x(first, range(chunks // 2, chunks))
    rim_in(second)
    attend(third, 1)
    pair_grads(second)
    weight_grad(second)
    grads_x(second, range(chunks // 2))
    await_pairs(fourth)
    attend(fourth, 0)
    rim_out(third)
    grads_x(second, range(chunks // 2, chunks))
    for k in range(chunks):
        rows_out(first, k)
    attend(fourth, 1)
    rim_out(fourth)
    rim_in(third)
    pair_grads(third)
    weight_grad(third)
    grads_x(third, range(chunks))
    for k in range(chunks):
        rows_out(second, k)
    rim_in(fourth)
    pair_grads(fourth)
    weight_grad(fourth)
    grads_x(fourth, range(chunks))

    dkv_mine = jnp.concatenate([dkvall[g, c].reshape(R, KV) for g in range(KVH)], axis=1)
    dots[tp] = jnp.zeros((R, 128), F32)
    inv_column = inv[:, :1]

    def hidden(i, _):
        columns = pl.ds(pl.multiple_of(i * tile, tile), tile)
        weight = wfull[:, :, columns].reshape(S * WR, tile)
        scaled = jnp.dot(dkv_mine, weight, preferred_element_type=F32) * (mask[:, columns].astype(F32) * DROP)
        wide = x_ref[:, columns].astype(F32)
        gains[0, :, columns] = jnp.sum(scaled * wide * inv_column, axis=0, keepdims=True)
        upstream = scaled * gain_row[:, columns]
        ups[:, columns] = upstream
        upstream = upstream * wide
        total = upstream[:, :128]
        for k in range(1, tile // 128):
            total = total + upstream[:, k * 128 : (k + 1) * 128]
        dots[tp] = dots[tp] + total
        return 0

    lax.fori_loop(0, F // tile, hidden, 0)
    for k in range(1, T):
        links.send(True, dots.at[tp], dots.at[tp], dot_recv.at[tp], sp, (tp + k) % T)
    links.send(True, gains.at[0], gains.at[1], gain_recv.at[1], mate, tp)
    links.arrive(gains.at[1], gain_recv.at[1], mate, tp)
    gains[2] = gains[0] + gains[1]
    for k in range(1, Z):
        links.send(True, gains.at[2], gains.at[2 + k], gain_recv.at[2 + k], at((z + k) % Z, x, c), tp)
    for k in range(chunks):
        rows_out(third, k)
    for k in range(chunks):
        rows_out(fourth, k)
    for k in range(1, T):
        links.arrive(dots.at[(tp + k) % T], dot_recv.at[(tp + k) % T], sp, (tp + k) % T)

    def finish_rows(i, _):
        r = pl.ds(pl.multiple_of(i * strip, strip), strip)
        total = dots[0, r, :]
        for t in range(1, T):
            total = total + dots[t, r, :]
        row_dot = jnp.sum(total, axis=1, keepdims=True)
        scale = inv[r, :1]
        ga_ref[r, :] = (
            scale * ups[r, :] - x_ref[r, :].astype(F32) * ((scale * scale * scale) * row_dot / D)
        ).astype(BF16)
        return 0

    lax.fori_loop(0, R // strip, finish_rows, 0)
    put_out(ga_ref, ga_hbm)
    total = gains[2]
    for k in range(1, Z):
        links.arrive(gains.at[2 + k], gain_recv.at[2 + k], mate, tp)
        total = total + gains[2 + k]
    gains[2 + Z] = total
    for k in range(1, X):
        links.send(True, gains.at[2 + Z], gains.at[2 + Z + k], gain_recv.at[2 + Z + k], at(z, (x + k) % X, c), tp)
    norm = (places * rows) ** (-0.5)

    for k in range(chunks):
        def result(columns, value):
            gw_ref[cut(k), columns] = value * norm

        sources = [(z + j) % Z for j in range(1, Z)]
        ends = (z == 0) | (z == Z - 1)

        def straight():
            for source in sources:
                links.arrive(zr.at[source, cut(k)], z_recv.at[source, k], mate, tp)
            fold(z, k, [zr.at[source] for source in sources], result)

        def beside():
            for source in (z - 1, z + 1):
                links.arrive(zr.at[source, cut(k)], z_recv.at[source, k], mate, tp)
            fold(z, k, [zr.at[z - 1], zr.at[z + 1]], result)

        pl.when(ends)(straight)
        pl.when(jnp.logical_not(ends))(beside)
        put_out(gw_ref.at[cut(k)], gw_hbm.at[cut(k)])
    for k in range(1, X):
        links.arrive(gains.at[2 + Z + k], gain_recv.at[2 + Z + k], mate, tp)
        total = total + gains[2 + Z + k]
    gg_ref[...] = total * norm
    links.drain()
    for copy in results:
        copy.wait()


def on_device(activations, norm_gain, keep_bits, key_value_weight, queries, segment, cotangent):
    S, T = lax.axis_size("sp"), lax.axis_size("tp")
    blocks, rows, F = activations.shape
    WR = key_value_weight.shape[0]
    Z = KVH
    X = S // (2 * Z)
    R = blocks * rows
    halo = 2 * -(-(DOC - 1) // (2 * rows))
    keys = rows * (halo + 1)
    chunks = WR // 16
    sends = chunks * (16 * X + 5) + 14 * (T - 1) + KVH * (2 * halo + 1) + X + 8
    shape = (S, T, X, Z, rows, F, WR, halo)
    vmem = pl.BlockSpec(memory_space=pltpu.VMEM)
    hbm = pl.BlockSpec(memory_space=pl.ANY)
    dma = pltpu.SemaphoreType.DMA
    wide = queries.shape[-1]
    out = pl.pallas_call(
        functools.partial(step_kernel, shape),
        in_specs=[hbm, vmem, hbm, hbm, hbm, vmem, hbm],
        out_specs=[hbm] * 4 + [vmem],
        out_shape=[
            jax.ShapeDtypeStruct((rows, wide), BF16),
            jax.ShapeDtypeStruct((rows, wide), BF16),
            jax.ShapeDtypeStruct((R, F), BF16),
            jax.ShapeDtypeStruct((WR, F), F32),
            jax.ShapeDtypeStruct((1, F), F32),
        ],
        scratch_shapes=[
            pltpu.VMEM((R, F), BF16),
            pltpu.VMEM((R, F // 8), jnp.int32),
            pltpu.VMEM((rows, wide), BF16),
            pltpu.VMEM((rows, wide), BF16),
            pltpu.VMEM((rows, wide), BF16),
            pltpu.VMEM((rows, wide), BF16),
            pltpu.VMEM((R, F), BF16),
            pltpu.VMEM((WR, F), F32),
            pltpu.VMEM((S, WR, F), BF16),
            pltpu.VMEM((2, R, F), BF16),
            pltpu.VMEM((R, F), BF16),
            pltpu.VMEM((R, 128), F32),
            pltpu.VMEM((T, R, 128), F32),
            pltpu.VMEM((T, R, 128), F32),
            pltpu.VMEM((KVH, T, rows, KV), F32),
            pltpu.VMEM((KVH, T, rows, KV), F32),
            pltpu.VMEM((halo + 1, KVH, rows, KV), BF16),
            pltpu.VMEM((KVH, halo, rows, KV), F32),
            pltpu.VMEM((KVH, halo // 2 + 1, rows, KV), F32),
            pltpu.VMEM((KVH, halo // 2, rows, KV), BF16),
            pltpu.VMEM((KVH, halo // 2, rows, KV), BF16),
            pltpu.VMEM((KVH, rows, KV), F32),
            pltpu.VMEM((KVH, 2, T, rows, KV), BF16),
            pltpu.VMEM((Z, WR, F), F32),
            pltpu.VMEM((Z, X - 1, WR, F), BF16),
            pltpu.VMEM((Z, X - 1, WR, F), BF16),
            pltpu.VMEM((Z, WR, F), BF16),
            pltpu.VMEM((Z, WR, F), BF16),
            pltpu.VMEM((Z, WR, F), BF16),
            pltpu.VMEM((R, F), F32),
            pltpu.VMEM((2 + X + Z, 1, F), F32),
            pltpu.VMEM((GROUP * rows, keys), BF16),
            pltpu.VMEM((GROUP * rows, keys), BF16),
            pltpu.VMEM((rows, keys), F32),
            pltpu.VMEM((1, F), F32),
            dma((sends,)),
            dma((5 + 2 * KVH + 1 + chunks,)),
            dma((S, WR // 16)),
            dma,
            dma((T,)),
            dma((T,)),
            dma((KVH, T)),
            dma((halo, KVH)),
            dma((KVH, halo // 2 + 1)),
            dma((KVH, halo // 2)),
            dma((KVH, T)),
            dma((KVH, T)),
            dma((Z, X, WR // 16)),
            dma((Z, WR // 16)),
            dma((Z, WR // 16)),
            dma((2 + X + Z,)),
        ],
        compiler_params=pltpu.CompilerParams(collective_id=0, has_side_effects=True, vmem_limit_bytes=63 * 2**20),
    )(
        activations.reshape(R, F),
        norm_gain,
        keep_bits.reshape(R, F // 8),
        key_value_weight,
        queries[0],
        segment.reshape(S * T, rows),
        cotangent[0],
    )
    attended, grad_queries, grad_activations, grad_weight, grad_gain = out
    return (
        attended[None],
        grad_queries[None],
        grad_activations.reshape(activations.shape),
        grad_weight,
        grad_gain.reshape(F),
    )


def solution(mesh):
    return jax.shard_map(
        on_device,
        mesh=mesh,
        in_specs=(
            P(None, "sp", "tp"),
            P("tp"),
            P(None, "sp", "tp"),
            P("sp", "tp"),
            P("tp", "sp", None),
            P(),
            P("tp", "sp", None),
        ),
        out_specs=(
            P("tp", "sp", None),
            P("tp", "sp", None),
            P(None, "sp", "tp"),
            P("sp", "tp"),
            P("tp"),
        ),
        check_vma=False,
    )
```

```python
import functools

import jax
import jax.numpy as jnp
import numpy as np
from jax import lax
from jax.experimental import pallas as pl
from jax.experimental.pallas import tpu as pltpu
from jax.sharding import PartitionSpec as P

D = 8192
HQ = 32
KVH = 4
HD = 128
DOC = 512
GROUP = 8
EPS = 1e-05
KEEP_RATE = 0.9
MASKED_SCORE = -1e30
SCALE = HD ** (-0.5)
DROP = float(np.float32(1.0) / np.float32(KEEP_RATE))
KV = 2 * HD
F32 = jnp.float32
BF16 = jnp.bfloat16
NT = (((1,), (1,)), ((), ()))
UNROLL = 1
BATCH = 4
LOG2E = 1.4426950408889634
TN = (((0,), (0,)), ((), ()))


class Links:
    def __init__(self, send_sems):
        self.send_sems = send_sems
        self.pending = []
        self.used = 0

    def send(self, cond, src, dst, recv_sem, sp, tp, again=False):
        self.used += not again
        sem = self.send_sems.at[self.used - 1]

        def make():
            return pltpu.make_async_remote_copy(
                src_ref=src,
                dst_ref=dst,
                send_sem=sem,
                recv_sem=recv_sem,
                device_id={"sp": sp, "tp": tp},
                device_id_type=pl.DeviceIdType.MESH,
            )

        self.pending.append((cond, make))
        when(cond, lambda: make().start())

    def arrive(self, dst, recv_sem, sp, tp):
        pltpu.make_async_remote_copy(
            src_ref=dst,
            dst_ref=dst,
            send_sem=self.send_sems.at[0],
            recv_sem=recv_sem,
            device_id={"sp": sp, "tp": tp},
            device_id_type=pl.DeviceIdType.MESH,
        ).wait_recv()

    def drain(self):
        for cond, make in self.pending:
            when(cond, lambda: make().wait_send())


def when(cond, body):
    if cond is True:
        body()
    else:
        pl.when(cond)(body)


def step_kernel(
    shape, x_hbm, gain_ref, bits_hbm, w_ref, query_hbm, seg_ref, cot_hbm,
    att_hbm, gq_hbm, ga_hbm, gw_hbm, gg_ref,
    x_ref, bits_ref, query_ref, cot_ref, att_ref, gq_ref, ga_ref, gw_ref,
    wfull, hall, mask, inv, squares, dots, kvp, kvr, kvh, rim, rimx, rimo, rimr, own_grad, dkvall,
    own32, xsend, xr, zs, zr, za, ups, gains, probs, grads, bias, gain_row,
    send_sems, local_sems, w_recv, h_recv, sq_recv, dot_recv, kv_recv, halo_recv, rimx_recv, rim_recv, dkv_recv, dkc_recv,
    x_recv, z_recv, a_recv, gain_recv,
):
    S, T, X, Z, rows, F, WR, halo = shape
    R = T * rows
    places = S * T
    sp, tp = lax.axis_index("sp"), lax.axis_index("tp")
    c = sp % 2
    x = sp // 2 % X
    z = sp // (2 * X)
    place = tp * S + sp
    at = lambda zz, xx, cc: (zz * X + xx) * 2 + cc
    mate = at(z, x, 1 - c)
    links = Links(send_sems)
    order = [g for pair in zip(range(Z - 1, Z // 2 - 1, -1), range(Z // 2)) for g in pair]
    chunks = WR // 16
    cut = lambda k: pl.ds(k * 16, 16)
    tile = min(512, F)
    strip = 16
    lanes = F // 128

    inputs = [
        pltpu.make_async_copy(w_ref, wfull.at[sp], local_sems.at[0]),
        pltpu.make_async_copy(x_hbm, x_ref, local_sems.at[1]),
        pltpu.make_async_copy(bits_hbm, bits_ref, local_sems.at[2]),
        pltpu.make_async_copy(query_hbm, query_ref, local_sems.at[3]),
        pltpu.make_async_copy(cot_hbm, cot_ref, local_sems.at[4]),
    ]
    for copy in inputs:
        copy.start()
    results = []

    def put_out(src, dst):
        copy = pltpu.make_async_copy(src, dst, local_sems.at[len(inputs) + len(results)])
        copy.start()
        results.append(copy)

    half = halo // 2
    barrier = pltpu.get_barrier_semaphore()

    def greet(cond, to_sp, to_tp):
        when(cond, lambda: pl.semaphore_signal(
            barrier, inc=1, device_id={"sp": to_sp, "tp": to_tp}, device_id_type=pl.DeviceIdType.MESH
        ))

    for k in range(1, Z):
        greet(True, at((z + k) % Z, x, c), tp)
    for k in range(1, X):
        greet(True, at(z, (x + k) % X, c), tp)
    greet(True, mate, tp)
    for k in range(1, T):
        greet(True, sp, (tp + k) % T)
    greeted = Z - 1 + X - 1 + 1 + T - 1
    for d in range(1, half + 1):
        for to in (place + 2 * d, place - 2 * d):
            inside = (to >= 0) & (to < places)
            greet(inside, (to + places) % S, (to + places) // S % T)
            greeted = greeted + jnp.where(inside, 1, 0)
    pl.semaphore_wait(barrier, greeted)
    inputs[0].wait()

    relayed, direct = order[:2], order[2:]

    def move_weight(cond, block, k, to, again=False):
        part = wfull.at[block, cut(k)]
        links.send(cond, part, part, w_recv.at[block, k], to, tp, again)

    def await_weight(cond, block, k):
        when(cond, lambda: links.arrive(wfull.at[block, cut(k)], w_recv.at[block, k], mate, tp))

    for g in relayed:
        for k in range(chunks):
            if g < Z - 1:
                move_weight(z == g, sp, k, at(z + 1, x, c))
            if g > 0:
                move_weight(z == g, sp, k, at(z - 1, x, c))
            for j in range(1, X):
                move_weight(z == g, sp, k, at(z, (x + j) % X, c))
    for k in range(chunks):
        move_weight(True, sp, k, mate)

    def weight_direct(g, k):
        for d in range(Z - 1, 0, -1):
            for to in (g - d, g + d):
                if 0 <= to < Z:
                    move_weight(z == g, sp, k, at(to, x, c))
        for j in range(1, X):
            move_weight(z == g, sp, k, at(z, (x + j) % X, c))

    def weight_in(g, k, relay=False):
        block = at(g, x, c)
        away = z != g
        await_weight(away, block, k)
        if relay:
            move_weight((z > g) & (z < Z - 1), block, k, at(z + 1, x, c))
            move_weight((z < g) & (z > 0), block, k, at(z - 1, x, c), True)
        for j in range(1, X):
            move_weight(away, block, k, at(z, (x + j) % X, c))
        move_weight(away, block, k, mate)

    def weight_x(g, k):
        for j in range(1, X):
            block = at(g, (x + j) % X, c)
            await_weight(True, block, k)
            move_weight(True, block, k, mate)

    def project(g):
        for k in range(chunks):
            for j in range(X):
                await_weight(True, at(g, j, 1 - c), k)
        weight = wfull[g * 2 * X : (g + 1) * 2 * X].reshape(2 * X * WR, F)
        part = lax.dot_general(hall[c], weight, NT, preferred_element_type=F32)
        for t in range(T):
            kvp[g, t] = part[t * rows : (t + 1) * rows]
        for k in range(1, T):
            to = (tp + k) % T
            links.send(True, kvp.at[g, to], kvr.at[g, tp], kv_recv.at[g, tp], sp, to)

    def square_rows(i, _):
        r = pl.ds(pl.multiple_of(i * strip, strip), strip)
        wide = x_ref[r, :].astype(F32)
        wide = wide * wide
        total = wide[:, :128]
        for k in range(1, lanes):
            total = total + wide[:, k * 128 : (k + 1) * 128]
        squares[tp, r, :] = total
        return 0

    inputs[1].wait()
    gain_row[...] = gain_ref[...].astype(F32).reshape(1, F)
    lax.fori_loop(0, R // strip, square_rows, 0)
    for k in range(1, T):
        links.send(True, squares.at[tp], squares.at[tp], sq_recv.at[tp], sp, (tp + k) % T)
    near = jnp.where(z < Z // 2, relayed[1], relayed[0])
    far = jnp.where(z < Z // 2, relayed[0], relayed[1])
    weight_in(near, 0, True)
    inputs[2].wait()
    words = min(128, F // 8)
    lane = lax.broadcasted_iota(jnp.int32, (words, words * 8), 1)
    expand = (lane // 8 == lax.broadcasted_iota(jnp.int32, (words, words * 8), 0)).astype(F32).astype(BF16)
    shifts = lax.broadcasted_iota(jnp.int32, (rows, words * 8), 1) % 8
    for w in range(F // 8 // words):
        def unpack(i, _):
            r = pl.ds(pl.multiple_of(i * rows, rows), rows)
            word = bits_ref[r, w * words : (w + 1) * words].astype(F32).astype(BF16)
            wide = jnp.dot(word, expand, preferred_element_type=F32).astype(jnp.int32)
            flag = jnp.bitwise_and(jnp.right_shift(wide, shifts), 1)
            mask[r, w * words * 8 : (w + 1) * words * 8] = flag.astype(F32).astype(BF16)
            return 0
        lax.fori_loop(0, T, unpack, 0)
    for k in range(1, T):
        links.arrive(squares.at[(tp + k) % T], sq_recv.at[(tp + k) % T], sp, (tp + k) % T)
    weight_in(near, 1, True)
    weight_in(far, 0, True)

    def norm_rows(i, _):
        r = pl.ds(pl.multiple_of(i * strip, strip), strip)
        total = squares[0, r, :]
        for t in range(1, T):
            total = total + squares[t, r, :]
        inv_rms = lax.rsqrt(jnp.sum(total, axis=1, keepdims=True) / D + EPS)
        inv[r, :] = jnp.broadcast_to(inv_rms, (strip, 128))
        wide = x_ref[r, :].astype(F32) * inv_rms * gain_row[...]
        hall[c, r, :] = (wide * (mask[r, :].astype(F32) * DROP)).astype(BF16)
        return 0

    lax.fori_loop(0, R // strip, norm_rows, 0)
    for k in range(2, chunks):
        weight_in(near, k, True)
        weight_in(far, k - 1, True)
    weight_in(far, chunks - 1, True)
    links.send(True, hall.at[c], hall.at[c], h_recv, mate, tp)

    zero = lambda ref: (lambda: ref.__setitem__(Ellipsis, jnp.zeros(ref.shape, ref.dtype)))
    for slot in range(halo):
        pl.when(place + slot < halo)(zero(kvh.at[slot]))
    for g in range(KVH):
        pl.when(c == 0)(zero(rimx.at[g, 0]))
        pl.when(c == 1)(zero(rimx.at[g, half]))
    keys = rows * (halo + 1)
    seg_rows = []
    for j in range(halo + 1):
        back = place - (halo - j)
        row = seg_ref[pl.ds(jnp.maximum(back, 0), 1), :]
        seg_rows.append(jnp.where(back >= 0, row, -1))
    seg_keys = jnp.concatenate(seg_rows, axis=1)
    seg_query = jnp.transpose(jnp.broadcast_to(seg_rows[halo].astype(F32), (rows, rows)))[:, :1]
    position = lax.broadcasted_iota(jnp.int32, (rows, keys), 0) + halo * rows
    other = lax.broadcasted_iota(jnp.int32, (rows, keys), 1)
    bias[...] = jnp.where((other <= position) & (seg_query == seg_keys.astype(F32)), 0.0, MASKED_SCORE)

    def sum_pairs(g):
        total = kvp[g, tp]
        for k in range(1, T):
            other = (tp + k) % T
            links.arrive(kvr.at[g, other], kv_recv.at[g, other], sp, other)
            total = total + kvr[g, other]
        kvh[halo, g] = total.astype(BF16)
        for d in range(1, half + 1):
            to = place + 2 * d
            links.send(to < places, kvh.at[halo, g], kvh.at[halo - 2 * d, g], halo_recv.at[halo - 2 * d, g], to % S, to // S % T)
        links.send(c == 0, kvh.at[halo, g], kvh.at[halo - 1, g], halo_recv.at[halo - 1, g], mate, tp)

    def share_pairs(g):
        for d in range(1, half + 1):
            slot = halo - 2 * d
            here = place >= 2 * d
            when(here, lambda: links.arrive(kvh.at[slot, g], halo_recv.at[slot, g], mate, tp))
            links.send(here & (c == 1), kvh.at[slot, g], kvh.at[slot + 1, g], halo_recv.at[slot + 1, g], mate, tp)
            if slot > 0:
                links.send(here & (c == 0), kvh.at[slot, g], kvh.at[slot - 1, g], halo_recv.at[slot - 1, g], mate, tp, True)

    def await_pairs(g):
        for slot in range(1, halo, 2):
            when(place + slot >= halo, lambda: links.arrive(kvh.at[slot, g], halo_recv.at[slot, g], mate, tp))

    def attend(g, part):
        heads = GROUP // 2

        pair = kvh[:, g].reshape(keys, KV)
        key_part, value_part = pair[:, :HD], pair[:, HD:]

        def some_heads(i, _):
            each = range(BATCH)
            n = [part * heads + i * BATCH + j for j in each]
            columns = [pl.ds(pl.multiple_of((g * GROUP + n[j]) * HD, HD), HD) for j in each]
            query = jnp.concatenate([query_ref[:, columns[j]] for j in each], axis=0)
            grad = jnp.concatenate([cot_ref[:, columns[j]] for j in each], axis=0)
            below = pl.ds(pl.multiple_of(n[0] * rows, rows), BATCH * rows)
            raw = lax.dot_general(query, key_part, NT, preferred_element_type=F32)
            grad_prob = lax.dot_general(grad, value_part, NT, preferred_element_type=F32)
            bias_all = jnp.concatenate([bias[...]] * BATCH, axis=0)
            scores = raw * (SCALE * LOG2E) + bias_all
            weights = jnp.exp2(scores - jnp.max(scores, axis=1, keepdims=True))
            prob = weights * (1.0 / jnp.sum(weights, axis=1, keepdims=True))
            low = prob.astype(BF16)
            probs[below, :] = low
            inner = jnp.sum(prob * grad_prob, axis=1, keepdims=True)
            grad_score = (prob * (grad_prob - inner)).astype(BF16)
            grads[below, :] = grad_score
            out = jnp.dot(low, value_part, preferred_element_type=F32).astype(BF16)
            grad_out = (jnp.dot(grad_score, key_part, preferred_element_type=F32) * SCALE).astype(BF16)
            for j in each:
                att_ref[:, columns[j]] = out[j * rows : (j + 1) * rows]
                gq_ref[:, columns[j]] = grad_out[j * rows : (j + 1) * rows]
            return 0

        lax.fori_loop(0, heads // BATCH, some_heads, 0, unroll=UNROLL)
        if part == 0:
            return
        wide = pl.ds(g * GROUP * HD, GROUP * HD)
        put_out(att_ref.at[:, wide], att_hbm.at[:, wide])
        put_out(gq_ref.at[:, wide], gq_hbm.at[:, wide])
        column = lambda ref, n: ref[:, (g * GROUP + n) * HD : (g * GROUP + n + 1) * HD]
        queries = jnp.concatenate([column(query_ref, n) for n in range(GROUP)], axis=0)
        cots = jnp.concatenate([column(cot_ref, n) for n in range(GROUP)], axis=0)
        grad_key = lax.dot_general(grads[...], queries, TN, preferred_element_type=F32) * SCALE
        grad_value = lax.dot_general(probs[...], cots, TN, preferred_element_type=F32)
        for j in range(halo):
            r = slice(j * rows, (j + 1) * rows)
            rim[g, j, :, :HD] = grad_key[r]
            rim[g, j, :, HD:] = grad_value[r]
        own_grad[g, :, :HD] = grad_key[halo * rows :]
        own_grad[g, :, HD:] = grad_value[halo * rows :]
        for j in range(1, halo, 2):
            low, high = (j - 1) // 2, (j + 1) // 2
            links.send(c == 0, rim.at[g, j], rimx.at[g, low], rimx_recv.at[g, low], mate, tp)
            links.send(c == 1, rim.at[g, j], rimx.at[g, high], rimx_recv.at[g, high], mate, tp, True)

    def rim_out(g):
        for i in range(half + 1):
            cond = True if 0 < i < half else ((c == 1) if i == 0 else (c == 0))
            when(cond, lambda: links.arrive(rimx.at[g, i], rimx_recv.at[g, i], mate, tp))
        for d in range(1, half + 1):
            slot = halo - 2 * d
            rimo[g, d - 1] = (rim[g, slot] + rimx[g, slot // 2]).astype(BF16)
            to = place - 2 * d
            links.send(to >= 0, rimo.at[g, d - 1], rimr.at[g, d - 1], rim_recv.at[g, d - 1], (to + places) % S, (to + places) // S % T)
        own_grad[g] = own_grad[g] + rimx[g, half]

    def rim_in(g):
        for d in range(1, half + 1):
            def add():
                links.arrive(rimr.at[g, d - 1], rim_recv.at[g, d - 1], mate, tp)
                own_grad[g] = own_grad[g] + rimr[g, d - 1].astype(F32)
            pl.when(place + 2 * d < places)(add)
        dkvall[g, c, tp] = own_grad[g].astype(BF16)
        mine = dkvall.at[g, c, tp]
        for k in range(1, T):
            links.send(True, mine, mine, dkv_recv.at[g, tp], sp, (tp + k) % T)
        links.send(True, mine, mine, dkc_recv.at[g, tp], mate, tp)

    def pair_grads(g):
        for k in range(1, T):
            other = (tp + k) % T
            part = dkvall.at[g, c, other]
            links.arrive(part, dkv_recv.at[g, other], sp, other)
            links.send(True, part, part, dkc_recv.at[g, other], mate, tp)

    def weight_grad(g):
        for t in range(T):
            links.arrive(dkvall.at[g, 1 - c, t], dkc_recv.at[g, t], mate, tp)
        if g == order[0]:
            links.arrive(hall.at[1 - c], h_recv, mate, tp)
        turned = jnp.transpose(dkvall[g].reshape(2 * R, KV).astype(F32))
        rest = turned.reshape(X, 2, WR, 2 * R)
        rest = jnp.where(c == 0, rest[:, 0], rest[:, 1])
        picked = []
        for k in range(X):
            piece = rest[k]
            for j in range(X):
                piece = jnp.where((x + k) % X == j, rest[j], piece)
            picked.append(piece)
        left = jnp.concatenate(picked, axis=0).astype(BF16)

        def outer(i, _):
            columns = pl.ds(pl.multiple_of(i * tile, tile), tile)
            right = hall[:, :, columns].reshape(2 * R, tile)
            part = jnp.dot(left, right, preferred_element_type=F32)
            own32[g, :, columns] = part[:WR]
            for k in range(1, X):
                xsend[g, k - 1, :, columns] = part[k * WR : (k + 1) * WR].astype(BF16)
            return 0

        lax.fori_loop(0, F // tile, outer, 0)

    def grads_x(g, pieces):
        for q in pieces:
            for k in range(1, X):
                links.send(True, xsend.at[g, k - 1, cut(q)], xr.at[g, k - 1, cut(q)], x_recv.at[g, k - 1, q], at(z, (x + k) % X, c), tp)

    def fold(g, k, extra, out):
        def body(i, _):
            columns = pl.ds(pl.multiple_of(i * tile, tile), tile)
            value = own32[g, cut(k), columns]
            for ref in extra:
                value = value + ref[cut(k), columns].astype(F32)
            out(columns, value)
            return 0
        lax.fori_loop(0, F // tile, body, 0)

    def rows_out(g, k):
        for j in range(1, X):
            links.arrive(xr.at[g, j - 1, cut(k)], x_recv.at[g, j - 1, k], mate, tp)
        parts = [xr.at[g, j - 1] for j in range(1, X)]

        def send_low(columns, value):
            zs[g, cut(k), columns] = value.astype(BF16)

        def keep(columns, value):
            own32[g, cut(k), columns] = value

        pl.when(z == g)(lambda: fold(g, k, parts, keep))
        if g in relayed:
            pl.when(z != g)(lambda: fold(g, k, parts, send_low))
            links.send(z != g, zs.at[g, cut(k)], zr.at[z, cut(k)], z_recv.at[z, k], at(g, x, c), tp)
            return
        for step, ends, passes in ((1, z == 0, (z > 0) & (z < g)), (-1, z == Z - 1, (z > g) & (z < Z - 1))):
            def add():
                links.arrive(za.at[g, cut(k)], a_recv.at[g, k], mate, tp)
                fold(g, k, parts + [za.at[g]], send_low)

            if (g if step > 0 else Z - 1 - g) > 0:
                pl.when(ends)(lambda: fold(g, k, parts, send_low))
                pl.when(passes)(add)
                going = (z < g) if step > 0 else (z > g)
                last = z + step == g
                links.send(going & last, zs.at[g, cut(k)], zr.at[z, cut(k)], z_recv.at[z, k], at(z + step, x, c), tp)
                links.send(going & (z + step != g), zs.at[g, cut(k)], za.at[g, cut(k)], a_recv.at[g, k], at(z + step, x, c), tp, True)

    first, second, third, fourth = order
    for k in range(chunks):
        weight_direct(third, k)
        weight_direct(fourth, k)
    inputs[3].wait()
    inputs[4].wait()
    for k in range(chunks):
        weight_x(first, k)
        weight_x(second, k)
    project(first)
    weight_in(third, 0)
    weight_in(third, 1)
    project(second)
    sum_pairs(first)
    for k in range(2, chunks - 1):
        weight_in(third, k)
    weight_x(third, 0)
    sum_pairs(second)
    share_pairs(first)
    for k in range(1, chunks // 2):
        weight_x(third, k)
    await_pairs(first)
    attend(first, 0)
    for k in range(max(chunks - 1, 2), chunks):
        weight_in(third, k)
    for k in range(chunks // 2):
        weight_in(fourth, k)
        weight_x(third, chunks // 2 + k)
    share_pairs(second)
    attend(first, 1)
    for k in range(chunks // 2, chunks):
        weight_in(fourth, k)
        weight_x(fourth, k - chunks // 2)
    await_pairs(second)
    rim_out(first)
    attend(second, 0)
    project(third)
    for k in range(chunks - chunks // 2, chunks):
        weight_x(fourth, k)
    rim_in(first)
    project(fourth)
    attend(second, 1)
    sum_pairs(third)
    sum_pairs(fourth)
    rim_out(second)
    pair_grads(first)
    weight_grad(first)
    share_pairs(third)
    grads_x(first, range(chunks // 2))
    await_pairs(third)
    attend(third, 0)
    share_pairs(fourth)
    grads_x(first, range(chunks // 2, chunks))
    rim_in(second)
    attend(third, 1)
    pair_grads(second)
    weight_grad(second)
    grads_x(second, range(chunks // 2))
    await_pairs(fourth)
    attend(fourth, 0)
    rim_out(third)
    grads_x(second, range(chunks // 2, chunks))
    for k in range(chunks):
        rows_out(first, k)
    attend(fourth, 1)
    rim_out(fourth)
    rim_in(third)
    pair_grads(third)
    weight_grad(third)
    grads_x(third, range(chunks))
    for k in range(chunks):
        rows_out(second, k)
    rim_in(fourth)
    pair_grads(fourth)
    weight_grad(fourth)
    grads_x(fourth, range(chunks))

    dkv_mine = jnp.concatenate([dkvall[g, c].reshape(R, KV) for g in range(KVH)], axis=1)
    dots[tp] = jnp.zeros((R, 128), F32)
    inv_column = inv[:, :1]

    def hidden(i, _):
        columns = pl.ds(pl.multiple_of(i * tile, tile), tile)
        weight = wfull[:, :, columns].reshape(S * WR, tile)
        scaled = jnp.dot(dkv_mine, weight, preferred_element_type=F32) * (mask[:, columns].astype(F32) * DROP)
        wide = x_ref[:, columns].astype(F32)
        gains[0, :, columns] = jnp.sum(scaled * wide * inv_column, axis=0, keepdims=True)
        upstream = scaled * gain_row[:, columns]
        ups[:, columns] = upstream
        upstream = upstream * wide
        total = upstream[:, :128]
        for k in range(1, tile // 128):
            total = total + upstream[:, k * 128 : (k + 1) * 128]
        dots[tp] = dots[tp] + total
        return 0

    lax.fori_loop(0, F // tile, hidden, 0)
    for k in range(1, T):
        links.send(True, dots.at[tp], dots.at[tp], dot_recv.at[tp], sp, (tp + k) % T)
    links.send(True, gains.at[0], gains.at[1], gain_recv.at[1], mate, tp)
    links.arrive(gains.at[1], gain_recv.at[1], mate, tp)
    gains[2] = gains[0] + gains[1]
    for k in range(1, Z):
        links.send(True, gains.at[2], gains.at[2 + k], gain_recv.at[2 + k], at((z + k) % Z, x, c), tp)
    for k in range(chunks):
        rows_out(third, k)
    for k in range(chunks):
        rows_out(fourth, k)
    for k in range(1, T):
        links.arrive(dots.at[(tp + k) % T], dot_recv.at[(tp + k) % T], sp, (tp + k) % T)

    def finish_rows(i, _):
        r = pl.ds(pl.multiple_of(i * strip, strip), strip)
        total = dots[0, r, :]
        for t in range(1, T):
            total = total + dots[t, r, :]
        row_dot = jnp.sum(total, axis=1, keepdims=True)
        scale = inv[r, :1]
        ga_ref[r, :] = (
            scale * ups[r, :] - x_ref[r, :].astype(F32) * ((scale * scale * scale) * row_dot / D)
        ).astype(BF16)
        return 0

    lax.fori_loop(0, R // strip, finish_rows, 0)
    put_out(ga_ref, ga_hbm)
    total = gains[2]
    for k in range(1, Z):
        links.arrive(gains.at[2 + k], gain_recv.at[2 + k], mate, tp)
        total = total + gains[2 + k]
    gains[2 + Z] = total
    for k in range(1, X):
        links.send(True, gains.at[2 + Z], gains.at[2 + Z + k], gain_recv.at[2 + Z + k], at(z, (x + k) % X, c), tp)
    norm = (places * rows) ** (-0.5)

    for k in range(chunks):
        def result(columns, value):
            gw_ref[cut(k), columns] = value * norm

        sources = [(z + j) % Z for j in range(1, Z)]
        ends = (z == 0) | (z == Z - 1)

        def straight():
            for source in sources:
                links.arrive(zr.at[source, cut(k)], z_recv.at[source, k], mate, tp)
            fold(z, k, [zr.at[source] for source in sources], result)

        def beside():
            for source in (z - 1, z + 1):
                links.arrive(zr.at[source, cut(k)], z_recv.at[source, k], mate, tp)
            fold(z, k, [zr.at[z - 1], zr.at[z + 1]], result)

        pl.when(ends)(straight)
        pl.when(jnp.logical_not(ends))(beside)
        put_out(gw_ref.at[cut(k)], gw_hbm.at[cut(k)])
    for k in range(1, X):
        links.arrive(gains.at[2 + Z + k], gain_recv.at[2 + Z + k], mate, tp)
        total = total + gains[2 + Z + k]
    gg_ref[...] = total * norm
    links.drain()
    for copy in results:
        copy.wait()


def hand_over(count, *refs):
    sources, targets, buffers = refs[:count], refs[count : 2 * count], refs[2 * count : 3 * count]
    in_sems, out_sems = refs[3 * count :]
    coming = [pltpu.make_async_copy(sources[i], buffers[i], in_sems.at[i]) for i in range(count)]
    going = [pltpu.make_async_copy(buffers[i], targets[i], out_sems.at[i]) for i in range(count)]
    for copy in coming:
        copy.start()
    for i in range(count):
        coming[i].wait()
        going[i].start()
    for copy in going:
        copy.wait()


def on_device(activations, norm_gain, keep_bits, key_value_weight, queries, segment, cotangent):
    S, T = lax.axis_size("sp"), lax.axis_size("tp")
    blocks, rows, F = activations.shape
    WR = key_value_weight.shape[0]
    Z = KVH
    X = S // (2 * Z)
    R = blocks * rows
    halo = 2 * -(-(DOC - 1) // (2 * rows))
    keys = rows * (halo + 1)
    chunks = WR // 16
    sends = chunks * (16 * X + 5) + 14 * (T - 1) + KVH * (2 * halo + 1) + X + 8
    shape = (S, T, X, Z, rows, F, WR, halo)
    vmem = pl.BlockSpec(memory_space=pltpu.VMEM)
    hbm = pl.BlockSpec(memory_space=pl.ANY)
    dma = pltpu.SemaphoreType.DMA
    wide = queries.shape[-1]
    out = pl.pallas_call(
        functools.partial(step_kernel, shape),
        in_specs=[hbm, vmem, hbm, hbm, hbm, vmem, hbm],
        out_specs=[hbm] * 4 + [vmem],
        out_shape=[
            jax.ShapeDtypeStruct((rows, wide), BF16),
            jax.ShapeDtypeStruct((rows, wide), BF16),
            jax.ShapeDtypeStruct((R, F), BF16),
            jax.ShapeDtypeStruct((WR, F), F32),
            jax.ShapeDtypeStruct((1, F), F32),
        ],
        scratch_shapes=[
            pltpu.VMEM((R, F), BF16),
            pltpu.VMEM((R, F // 8), jnp.int32),
            pltpu.VMEM((rows, wide), BF16),
            pltpu.VMEM((rows, wide), BF16),
            pltpu.VMEM((rows, wide), BF16),
            pltpu.VMEM((rows, wide), BF16),
            pltpu.VMEM((R, F), BF16),
            pltpu.VMEM((WR, F), F32),
            pltpu.VMEM((S, WR, F), BF16),
            pltpu.VMEM((2, R, F), BF16),
            pltpu.VMEM((R, F), BF16),
            pltpu.VMEM((R, 128), F32),
            pltpu.VMEM((T, R, 128), F32),
            pltpu.VMEM((T, R, 128), F32),
            pltpu.VMEM((KVH, T, rows, KV), F32),
            pltpu.VMEM((KVH, T, rows, KV), F32),
            pltpu.VMEM((halo + 1, KVH, rows, KV), BF16),
            pltpu.VMEM((KVH, halo, rows, KV), F32),
            pltpu.VMEM((KVH, halo // 2 + 1, rows, KV), F32),
            pltpu.VMEM((KVH, halo // 2, rows, KV), BF16),
            pltpu.VMEM((KVH, halo // 2, rows, KV), BF16),
            pltpu.VMEM((KVH, rows, KV), F32),
            pltpu.VMEM((KVH, 2, T, rows, KV), BF16),
            pltpu.VMEM((Z, WR, F), F32),
            pltpu.VMEM((Z, X - 1, WR, F), BF16),
            pltpu.VMEM((Z, X - 1, WR, F), BF16),
            pltpu.VMEM((Z, WR, F), BF16),
            pltpu.VMEM((Z, WR, F), BF16),
            pltpu.VMEM((Z, WR, F), BF16),
            pltpu.VMEM((R, F), F32),
            pltpu.VMEM((2 + X + Z, 1, F), F32),
            pltpu.VMEM((GROUP * rows, keys), BF16),
            pltpu.VMEM((GROUP * rows, keys), BF16),
            pltpu.VMEM((rows, keys), F32),
            pltpu.VMEM((1, F), F32),
            dma((sends,)),
            dma((5 + 2 * KVH + 1 + chunks,)),
            dma((S, WR // 16)),
            dma,
            dma((T,)),
            dma((T,)),
            dma((KVH, T)),
            dma((halo, KVH)),
            dma((KVH, halo // 2 + 1)),
            dma((KVH, halo // 2)),
            dma((KVH, T)),
            dma((KVH, T)),
            dma((Z, X, WR // 16)),
            dma((Z, WR // 16)),
            dma((Z, WR // 16)),
            dma((2 + X + Z,)),
        ],
        compiler_params=pltpu.CompilerParams(collective_id=0, has_side_effects=True, vmem_limit_bytes=63 * 2**20),
    )(
        activations.reshape(R, F),
        norm_gain,
        keep_bits.reshape(R, F // 8),
        key_value_weight,
        queries[0],
        segment.reshape(S * T, rows),
        cotangent[0],
    )
    out = pl.pallas_call(
        functools.partial(hand_over, len(out)),
        in_specs=[hbm] * len(out),
        out_specs=[hbm] * len(out),
        out_shape=[jax.ShapeDtypeStruct(o.shape, o.dtype) for o in out],
        scratch_shapes=[pltpu.VMEM(o.shape, o.dtype) for o in out] + [dma((len(out),)), dma((len(out),))],
        compiler_params=pltpu.CompilerParams(vmem_limit_bytes=60 * 2**20),
    )(*out)
    attended, grad_queries, grad_activations, grad_weight, grad_gain = out
    return (
        attended[None],
        grad_queries[None],
        grad_activations.reshape(activations.shape),
        grad_weight,
        grad_gain.reshape(F),
    )


def solution(mesh):
    return jax.shard_map(
        on_device,
        mesh=mesh,
        in_specs=(
            P(None, "sp", "tp"),
            P("tp"),
            P(None, "sp", "tp"),
            P("sp", "tp"),
            P("tp", "sp", None),
            P(),
            P("tp", "sp", None),
        ),
        out_specs=(
            P("tp", "sp", None),
            P("tp", "sp", None),
            P(None, "sp", "tp"),
            P("sp", "tp"),
            P("tp"),
        ),
        check_vma=False,
    )
```
